32 devices in a mesh: dp: 16 (over z, y, core), tensor: 2 (over x).
Axes of the slice: x: 2, y: 2, z: 4, core: 2. Of those that a mesh axis runs over, the one named last changes fastest.
Arguments:
- activations: bfloat16 [4096, 27648], P('dp', 'tensor'), may hold values from -6 to 6
- output_gradient: bfloat16 [4096, 5120], P('dp', 'tensor'), may hold values from -6 to 6
- adapter_a: bfloat16 [2, 13824, 128], P('tensor', 'dp'), may hold values from -0.0390625 to 0.0390625
- adapter_b: bfloat16 [128, 5120], P(None, 'tensor'), may hold values from -0.078125 to 0.078125
- log_ratio: float32 [4096], P('dp'), may hold values from -1.5 to 1.5
- lengths: int32 [1, 16], replicated, may hold values from 1 to 256, as said below
- rewards: int32 [1, 16], replicated, may hold values from 0 to 10
Outputs:
- grad_a: float32 [2, 13824, 128], P('tensor', 'dp')
- adapter_b_gradient: float32 [128, 5120], P(None, 'tensor')
- loss: float32 [], replicated
The draws below stay inside these ranges and needn't reach their ends.
Inputs may be any that keep to these rules, and one draw needn't show every extreme that they name: `lengths`: in every group some rollout has length 256.
All inputs are finite; a program needn't handle non-finite values.
Results may differ from the reference program's by a relative error of at most 0.0067.
Values may be sent and summed in bfloat16 or wider, within the bound.
A program may use at most 64 MiB of HBM per device.

```python
import jax
import jax.numpy as jnp
from jax import lax

D = 5120
FF = 27648
R = 128
ROLLOUTS = 16
MOST = 256
GROUPS = 1
TOKENS = 4096
TP_BLOCKS = 2
FF_TP = 13824


def draw_lengths(key, part):
    first_key, second_key = jax.random.split(jax.random.fold_in(key, 17))
    base = jax.random.randint(first_key, (GROUPS, ROLLOUTS), 1, MOST + 1)
    chosen = jax.random.randint(second_key, (GROUPS, 1), 0, ROLLOUTS)
    column_ids = jnp.arange(ROLLOUTS)[None, :]
    return jnp.where(column_ids == chosen, MOST, base).astype(jnp.int32)


def with_ends(drawn, rng, low, largest):
    shape = drawn.shape
    place = [jax.random.randint(jax.random.fold_in(rng, axis), (), 0, shape[axis]) for axis in range(len(shape))]
    drawn = drawn.at[tuple(place)].set(low)
    longest = shape.index(max(shape))
    place[longest] = (place[longest] + 1) % shape[longest]
    return drawn.at[tuple(place)].set(largest)


def strengthened(result, key, source, target, blocks, factor):
    owner, partner = [(jnp.arange(result.shape[axis_at]) // (result.shape[axis_at] // blocks)).reshape([-1 if axis == axis_at else 1 for axis in range(result.ndim)]) for axis_at in (source, target)]
    chosen = jax.random.permutation(key, blocks)[partner]
    strong = (owner == chosen) | (owner == (partner + blocks // 2) % blocks)
    return jnp.where(strong, factor * result, result)


def levels(stream_key, dims, cuts, low, top_value):
    def one(position, shards_of):
        heights = jax.random.uniform(jax.random.fold_in(jax.random.fold_in(stream_key, 6), position), (shards_of,), jnp.float32, low / len(cuts), top_value / len(cuts))
        return jnp.repeat(jnp.exp(heights), dims[position] // shards_of).reshape((-1,) + (1,) * (len(dims) - position - 1))

    level = one(*cuts[0])
    for cut in cuts[1:]:
        level = level * one(*cut)
    return level


def centred(rng, shape, deviation, limit, cuts=(), kind=jnp.bfloat16):
    level = levels(rng, shape, cuts, -0.22, 0.18) if cuts else 1.0
    values = jax.random.normal(rng, shape, jnp.float32) * deviation * level
    return jnp.minimum(jnp.maximum(values, -limit), limit).astype(kind)


def noise_with(own_key, shape, scale, bound, pieces, heavy, kind=jnp.bfloat16):
    entries = scale * jax.random.normal(own_key, shape, jnp.float32)
    if pieces:
        entries = entries * levels(own_key, shape, pieces, -0.22, 0.18)
    return jnp.clip(strengthened(entries, jax.random.fold_in(own_key, 3), *heavy), -bound, bound).astype(kind)


def setup_inputs(seed: int = 0) -> dict:
    streams_of = jax.random.split(jax.random.key(seed), 8)
    activations = noise_with(streams_of[0], (TOKENS, FF), 1.0, 6.0, ((0, 16), (1, 2)), (0, 1, 16, 2.0))
    output_gradient = centred(streams_of[1], (TOKENS, D), 1.0, 6.0, ((0, 16), (1, 2)))
    adapter_a = centred(streams_of[2], (TP_BLOCKS, FF_TP, R), FF ** -0.5, 0.0390625, ((0, 2), (1, 16)))
    adapter_b = centred(streams_of[3], (R, D), D ** -0.5, 0.078125, ((1, 2),))
    log_ratio = centred(streams_of[4], (TOKENS,), 0.25, 1.5, ((0, 16),), jnp.float32)
    lengths = draw_lengths(jax.random.fold_in(streams_of[7], 71), 0)
    rewards = with_ends(jax.random.randint(streams_of[6], (GROUPS, ROLLOUTS), 0, 11), jax.random.fold_in(streams_of[6], 1), 0, 10).astype(jnp.int32)
    return dict(activations=activations, output_gradient=output_gradient, adapter_a=adapter_a, adapter_b=adapter_b, log_ratio=log_ratio, lengths=lengths, rewards=rewards)


clip_eps = 0.2
adapter_scale_factor = 2.0

def token_terms(length_row, reward_row, log_ratio, offset):
    reward = reward_row.astype(jnp.float32)
    center = jnp.mean(reward)
    spread = jnp.mean((reward - center) * (reward - center))
    advantage = (reward - center) / jnp.sqrt(spread + 1.0)
    ends = jnp.cumsum(length_row).astype(jnp.int32)
    starts = (ends - length_row).astype(jnp.int32)
    slots = jnp.arange(log_ratio.shape[0], dtype=jnp.int32) + offset
    member = ((slots[None, :] >= starts[:, None]) & (slots[None, :] < ends[:, None])).astype(jnp.float32)
    live = lax.optimization_barrier(jnp.sum(member, axis=0))
    token_adv = lax.optimization_barrier(jnp.sum(member * advantage[:, None], axis=0))
    ratio = jnp.exp(log_ratio)
    unclipped = ratio * token_adv
    clipped = jnp.clip(ratio, 1.0 - clip_eps, 1.0 + clip_eps) * token_adv
    token_loss = -jnp.minimum(unclipped, clipped)
    slope = jnp.where(unclipped <= clipped, -unclipped, jnp.zeros_like(unclipped))
    return (live * slope, jnp.sum(live * token_loss), jnp.sum(live))

def reference(activations, output_gradient, adapter_a, adapter_b, log_ratio, lengths, rewards):
    groups = lengths.shape[0]
    offsets = jnp.zeros((groups,), jnp.int32)
    token_coefficient, loss_parts, live_parts = jax.vmap(token_terms)(lengths, rewards, log_ratio.reshape(groups, -1), offsets)
    token_coefficient = token_coefficient.reshape(-1)
    ratio_multiplier = groups / jnp.sum(live_parts)
    a_whole = adapter_a.reshape(-1, adapter_a.shape[2])
    low_rank = jnp.dot(activations, a_whole, preferred_element_type=jnp.float32)
    backward_projection = jnp.dot(output_gradient, adapter_b.T, preferred_element_type=jnp.float32)
    error_rows = (adapter_scale_factor * token_coefficient[:, None] * backward_projection).astype(jnp.bfloat16)
    grad_a = ratio_multiplier * lax.dot_general(activations, error_rows, (((0,), (0,)), ((), ())), preferred_element_type=jnp.float32)
    weighted_error = token_coefficient[:, None] * low_rank
    adapter_b_gradient = ratio_multiplier * adapter_scale_factor * jnp.dot(weighted_error.T, output_gradient.astype(jnp.float32), precision=lax.Precision.HIGHEST)
    loss = ratio_multiplier * jnp.sum(loss_parts)
    return (grad_a.reshape(adapter_a.shape), adapter_b_gradient, loss)
```

```python
import functools

import jax
import jax.numpy as jnp
from jax import lax
from jax.experimental import pallas as pl
from jax.experimental.pallas import tpu as pltpu
from jax.sharding import PartitionSpec as P

clip_eps = 0.2
adapter_scale_factor = 2.0


def token_terms(length_row, reward_row, log_ratio, offset):
    reward = reward_row.astype(jnp.float32)
    center = jnp.mean(reward)
    spread = jnp.mean((reward - center) * (reward - center))
    advantage = (reward - center) / jnp.sqrt(spread + 1.0)
    ends = jnp.cumsum(length_row)
    starts = ends - length_row
    slots = jnp.arange(log_ratio.shape[0], dtype=jnp.int32) + offset
    member = ((slots[None, :] >= starts[:, None]) & (slots[None, :] < ends[:, None])).astype(
        jnp.float32
    )
    live = jnp.sum(member, axis=0)
    token_adv = jnp.sum(member * advantage[:, None], axis=0)
    ratio = jnp.exp(log_ratio)
    unclipped = ratio * token_adv
    clipped = jnp.clip(ratio, 1.0 - clip_eps, 1.0 + clip_eps) * token_adv
    token_loss = -jnp.minimum(unclipped, clipped)
    slope = jnp.where(unclipped <= clipped, -unclipped, jnp.zeros_like(unclipped))
    return (live * slope, jnp.sum(live * token_loss), jnp.sum(live))


def plain_local(activations, output_gradient, adapter_a, adapter_b, log_ratio, lengths, rewards):
    tokens = activations.shape[0]
    groups = lengths.shape[0]
    per_group = lax.axis_size("dp") // groups
    position = lax.axis_index("dp")
    group_id = position // per_group
    offset = position % per_group * tokens
    length_row = lax.dynamic_index_in_dim(lengths, group_id, 0, keepdims=False)
    reward_row = lax.dynamic_index_in_dim(rewards, group_id, 0, keepdims=False)
    token_coefficient, loss_local, live_count = token_terms(
        length_row, reward_row, log_ratio, offset
    )
    columns = activations
    partial_low = jnp.dot(
        columns,
        lax.all_gather(adapter_a, "dp", axis=1, tiled=True)[0],
        preferred_element_type=jnp.float32,
    )
    partial_back = lax.dot_general(
        output_gradient, adapter_b, (((1,), (1,)), ((), ())), preferred_element_type=jnp.float32
    )
    low_rank, backward_projection = lax.psum((partial_low, partial_back), "tensor")
    error_rows = (adapter_scale_factor * token_coefficient[:, None] * backward_projection).astype(
        jnp.bfloat16
    )
    weighted_error = token_coefficient[:, None] * low_rank
    local_adapter_b_gradient = adapter_scale_factor * jnp.einsum(
        "tr,td->rd",
        weighted_error,
        output_gradient.astype(jnp.float32),
        precision=lax.Precision.HIGHEST,
    )
    columns = activations
    grad_a = lax.psum_scatter(
        lax.dot_general(
            columns, error_rows, (((0,), (0,)), ((), ())), preferred_element_type=jnp.float32
        ),
        "dp",
        scatter_dimension=0,
        tiled=True,
    )
    grad_b_sum, loss_sum, live_sum = lax.psum(
        (local_adapter_b_gradient, loss_local, live_count), "dp"
    )
    factor = groups / live_sum
    return ((factor * grad_a)[None], factor * grad_b_sum, factor * loss_sum)


MESH = pl.DeviceIdType.MESH
f32, bf16 = jnp.float32, jnp.bfloat16


def tile_of(total, most):
    return max(k for k in range(128, most + 1, 128) if total % k == 0)


def fused_kernel(
    n, groups, rollouts,
    act_hbm, grad_hbm, a_hbm, b_hbm, ratio_hbm, len_hbm, rew_hbm,
    out_a, out_b, out_loss,
    ratio_ref, len_ref, rew_ref,
    act, grad, b_mat, a_all, part, rs1, rs2, rs3, xs, xr, coef, err,
    gb, gbs, gb1, gb2s, gb2, gb3s, gb3, fin, ls, l1, l2, lz,
    loc, ag_s, ag_r, rs1_s, rs1_r, rs2_s, rs2_r, rs3_s, rs3_r, x_s, x_r,
    g_s, g_r, gz_s, gz_r, fz_s, fz_r, l_s, l_r, lz_s, lz_r,
):
    depth = n // 4
    p = lax.axis_index("dp")
    t = lax.axis_index("tensor")
    c, y, z = p % 2, (p // 2) % 2, p // 4
    tokens, ff = act.shape
    rows, rank = a_hbm.shape

    def at(zz, yy, cc):
        return (zz * 2 + yy) * 2 + cc

    def turn(k):
        return lax.rem(z + (k + depth), depth)

    def block(ref, q):
        return ref.at[pl.ds(pl.multiple_of(q * rows, 16), rows)]

    def remote(s, d, ss, rs, dev, tensor=None):
        return pltpu.make_async_remote_copy(
            src_ref=s, dst_ref=d, send_sem=ss, recv_sem=rs,
            device_id=(dev, t if tensor is None else tensor), device_id_type=MESH,
        )

    core, side = at(z, y, 1 - c), at(z, 1 - y, c)
    zs = [turn(k) for k in range(depth)]
    peer = [at(zs[k], y, c) for k in range(depth)]

    load_a = pltpu.make_async_copy(a_hbm, block(a_all, p), loc.at[0])
    load_g = pltpu.make_async_copy(grad_hbm, grad, loc.at[1])
    load_b = pltpu.make_async_copy(b_hbm, b_mat, loc.at[2])
    load_x = pltpu.make_async_copy(act_hbm, act, loc.at[3])
    small = [
        pltpu.make_async_copy(s, d, loc.at[4 + i])
        for i, (s, d) in enumerate(((ratio_hbm, ratio_ref), (len_hbm, len_ref), (rew_hbm, rew_ref)))
    ]
    barrier = pltpu.get_barrier_semaphore()
    for dev in [core, side] + peer[1:]:
        pl.semaphore_signal(barrier, inc=1, device_id=(dev, t), device_id_type=MESH)
    pl.semaphore_signal(barrier, inc=1, device_id=(p, 1 - t), device_id_type=MESH)
    for copy in [load_a, load_g, load_b] + small + [load_x]:
        copy.start()
    load_g.wait()
    load_b.wait()
    xs[0] = lax.dot_general(grad[...], b_mat[...], (((1,), (1,)), ((), ())), preferred_element_type=f32)
    load_a.wait()
    pl.semaphore_wait(barrier, depth + 2)

    sent = []

    def go(copy):
        copy.start()
        sent.append(copy)
        return copy

    count = [0]

    def gather_send(q, dev):
        go(remote(block(a_all, q), block(a_all, q), ag_s.at[count[0]], ag_r.at[q], dev))
        count[0] += 1

    def gather_wait(q):
        remote(block(a_all, q), block(a_all, q), ag_s.at[0], ag_r.at[q], core).wait_recv()

    far = sorted(range(1, depth), key=lambda k: -min(k, depth - k))
    gather_send(p, side)
    for k in far:
        gather_send(p, peer[k])
    gather_send(p, core)

    back = go(remote(xs.at[0], xr.at[0], x_s.at[0], x_r.at[0], p, 1 - t))

    for copy in small:
        copy.wait()
    per_group = n // groups
    group = p // per_group
    offset = (p % per_group) * tokens
    slots = (
        lax.broadcasted_iota(jnp.int32, ratio_ref.shape, 0) * 128
        + lax.broadcasted_iota(jnp.int32, ratio_ref.shape, 1)
        + offset
    )
    live_total = jnp.int32(0)
    live = jnp.zeros(ratio_ref.shape, f32)
    token_adv = jnp.zeros(ratio_ref.shape, f32)
    for g in range(groups):
        here = jnp.full((1, 128), (group == g).astype(f32))
        reward = [jnp.full((1, 128), rew_ref[g, i]).astype(f32) for i in range(rollouts)]
        center = sum(reward) / rollouts
        spread = sum((r - center) * (r - center) for r in reward) / rollouts
        scale = jnp.sqrt(spread + 1.0)
        end = jnp.int32(0)
        for i in range(rollouts):
            start = end
            end = end + len_ref[g, i]
            member = ((slots >= start) & (slots < end)).astype(f32) * here
            live = live + member
            token_adv = token_adv + member * ((reward[i] - center) / scale)
        live_total = live_total + jnp.minimum(end, per_group * tokens)
    ratio = jnp.exp(ratio_ref[...])
    unclipped = ratio * token_adv
    clipped = jnp.clip(ratio, 1.0 - clip_eps, 1.0 + clip_eps) * token_adv
    token_loss = -jnp.minimum(unclipped, clipped)
    slope = jnp.where(unclipped <= clipped, -unclipped, jnp.zeros_like(unclipped))
    weight = live * slope
    for i in range(tokens // 128):
        coef[pl.ds(i * 128, 128), :] = jnp.broadcast_to(weight[i : i + 1, :], (128, 128)).T
    factor = groups / jnp.full((1, 128), live_total).astype(f32)
    loss_part = jnp.sum(jnp.sum(live * token_loss, axis=1, keepdims=True), axis=0, keepdims=True)

    ls[0] = jnp.broadcast_to(loss_part, (8, 128))
    first = go(remote(ls.at[0], l1, l_s.at[0], l_r.at[0], core))

    back.wait_recv()
    err[...] = (adapter_scale_factor * coef[...] * (xs[0] + xr[0])).astype(bf16)

    load_x.wait()
    tile = tile_of(ff, 1536)
    steps = ff // tile

    def partial_rows(i, _):
        cols = pl.ds(pl.multiple_of(i * tile, 128), tile)
        part[cols, :] = lax.dot_general(
            act[:, cols], err[...], (((0,), (0,)), ((), ())), preferred_element_type=f32
        ).astype(bf16)
        return 0

    near = [depth - k for k in far][::-1]
    for j, k in enumerate(near):
        lax.fori_loop(j * steps // len(near), (j + 1) * steps // len(near), partial_rows, 0)
        q = peer[k]
        gather_wait(q)
        gather_send(q, side)
        gather_send(q, core)

    order = far + [0]
    first_stage = {}
    for yy in (1, 0):
        for k in order:
            yv = 1 - y if yy else y
            i = k * 2 + yy
            first_stage[k, yy] = go(
                remote(block(part, at(zs[k], yv, 1 - c)), rs1.at[i], rs1_s.at[i], rs1_r.at[i], core)
            )

    first.wait_recv()
    ls[1] = ls[0] + l1[...]
    second = go(remote(ls.at[1], l2, l_s.at[1], l_r.at[1], side))

    second_stage = {}
    for k in order:
        first_stage[k, 1].wait_recv()
        own = block(part, at(zs[k], 1 - y, c))
        own[...] = (own[...].astype(f32) + rs1[k * 2 + 1].astype(f32)).astype(bf16)
        second_stage[k] = go(remote(own, rs2.at[k], rs2_s.at[k], rs2_r.at[k], side))

    second.wait_recv()
    lz[z] = ls[1] + l2[...]
    third = [go(remote(lz.at[z], lz.at[z], lz_s.at[k], lz_r.at[k], peer[k])) for k in range(1, depth)]

    for k in [0] + near:
        q = at(zs[k], 1 - y, c)
        gather_wait(q)
        gather_send(q, core)
    for k in range(depth):
        gather_wait(at(zs[k], y, 1 - c))
    for k in range(depth):
        gather_wait(at(zs[k], 1 - y, 1 - c))

    def low_rows(i, total):
        cols = pl.ds(pl.multiple_of(i * tile, 128), tile)
        return total + jnp.dot(act[:, cols], a_all[cols, :], preferred_element_type=f32)

    xs[1] = lax.fori_loop(0, steps, low_rows, jnp.zeros((tokens, rank), f32))
    low = go(remote(xs.at[1], xr.at[1], x_s.at[1], x_r.at[1], p, 1 - t))

    third_stage = {}
    for k in far:
        first_stage[k, 0].wait_recv()
        second_stage[k].wait_recv()
        own = block(part, at(zs[k], y, c))
        own[...] = (
            own[...].astype(f32) + rs1[k * 2].astype(f32) + rs2[k].astype(f32)
        ).astype(bf16)
        third_stage[k] = go(remote(own, rs3.at[k], rs3_s.at[k], rs3_r.at[k], peer[k]))

    low.wait_recv()
    weighted = coef[...] * (xs[1] + xr[1])
    high = weighted.astype(bf16)
    rest = weighted - high.astype(f32)
    middle = rest.astype(bf16)
    last = (rest - middle.astype(f32)).astype(bf16)
    width = grad.shape[1]
    wide = tile_of(width, 640)
    for i in range(width // wide):
        cols = pl.ds(i * wide, wide)
        g = grad[:, cols]
        total = sum(
            lax.dot_general(w, g, (((0,), (0,)), ((), ())), preferred_element_type=f32)
            for w in (last, middle, high)
        )
        gb[:, cols] = total
        gbs[:, cols] = total.astype(bf16)

    half, quarter, chunk = rank // 2, rank // 4, width // depth
    lane = pl.multiple_of(c * half, 16)
    other = pl.multiple_of((1 - c) * half, 16)
    one = go(remote(gbs.at[pl.ds(other, half)], gb1, g_s.at[0], g_r.at[0], core))
    one.wait_recv()
    away = pl.multiple_of((1 - y) * quarter, 16)
    stay = pl.multiple_of(y * quarter, 16)
    mine = pl.multiple_of(lane + stay, 16)
    gb2s[...] = (
        gb[pl.ds(pl.multiple_of(lane + away, 16), quarter), :] + gb1[pl.ds(away, quarter), :].astype(f32)
    ).astype(bf16)
    two = go(remote(gb2s, gb2, g_s.at[1], g_r.at[1], side))

    first_stage[0, 0].wait_recv()
    second_stage[0].wait_recv()
    total = block(part, p)[...].astype(f32) + rs1[0].astype(f32) + rs2[0].astype(f32)
    out_a[...] = total

    two.wait_recv()
    total = (
        gb[pl.ds(mine, quarter), :]
        + gb1[pl.ds(stay, quarter), :].astype(f32)
        + gb2[...].astype(f32)
    )
    gb3s[...] = total.astype(bf16)
    gb[pl.ds(mine, quarter), :] = total

    def chunk_of(zz):
        return pl.ds(pl.multiple_of(zz * chunk, 128), chunk)

    three = {
        k: go(remote(gb3s.at[:, chunk_of(zs[k])], gb3.at[k], gz_s.at[k], gz_r.at[k], peer[k]))
        for k in far
    }

    for k in far:
        third_stage[k].wait_recv()
        out_a[...] = out_a[...] + rs3[k].astype(f32)
    out_a[...] = factor * out_a[...]
    for copy in third:
        copy.wait_recv()
    total = lz[0]
    for i in range(1, depth):
        total = total + lz[i]
    out_loss[...] = factor * total

    for k in far:
        three[k].wait_recv()
    total = gb[pl.ds(mine, quarter), chunk_of(z)]
    for k in far:
        total = total + gb3[k].astype(f32)
    scaled = jnp.full((1, 128), adapter_scale_factor) * factor
    fin[pl.ds(mine, quarter), chunk_of(z)] = (scaled[:, :1] * total).astype(bf16)

    piece = fin.at[pl.ds(mine, quarter), chunk_of(z)]
    four = {k: go(remote(piece, piece, fz_s.at[k], fz_r.at[k], peer[k])) for k in far}
    for k in far:
        four[k].wait_recv()
    piece = fin.at[pl.ds(mine, quarter)]
    five = go(remote(piece, piece, g_s.at[2], g_r.at[2], side))
    five.wait_recv()
    piece = fin.at[pl.ds(lane, half)]
    six = go(remote(piece, piece, g_s.at[3], g_r.at[3], core))
    six.wait_recv()
    out_b[...] = fin[...].astype(f32)
    for copy in sent:
        copy.wait_send()


def finish_kernel(a_in, b_in, loss_in, a_out, b_out, loss_out, sems):
    copies = [
        pltpu.make_async_copy(s, d, sems.at[i])
        for i, (s, d) in enumerate(((a_in, a_out), (b_in, b_out)))
    ]
    for copy in copies:
        copy.start()
    loss_out[0, 0] = loss_in[0, 0]
    for copy in copies:
        copy.wait()


def fused_local(activations, output_gradient, adapter_a, adapter_b, log_ratio, lengths, rewards):
    n = lax.axis_size("dp")
    depth = n // 4
    tokens, ff = activations.shape
    rows, rank = adapter_a.shape[1:]
    width = output_gradient.shape[1]
    dma = pltpu.SemaphoreType.DMA
    vmem, anywhere = pl.BlockSpec(memory_space=pltpu.VMEM), pl.BlockSpec(memory_space=pl.ANY)
    scalars = pl.BlockSpec(memory_space=pltpu.SMEM)
    hbm = pl.BlockSpec(memory_space=pltpu.HBM)
    quarter, chunk = rank // 4, width // depth
    grad_a, grad_b, loss = pl.pallas_call(
        functools.partial(fused_kernel, n, lengths.shape[0], lengths.shape[1]),
        out_shape=(
            jax.ShapeDtypeStruct((rows, rank), f32),
            jax.ShapeDtypeStruct((rank, width), f32),
            jax.ShapeDtypeStruct((8, 128), f32),
        ),
        in_specs=[hbm] * 7,
        out_specs=(vmem, vmem, vmem),
        scratch_shapes=[
            pltpu.VMEM((tokens // 128, 128), f32),
            pltpu.SMEM(lengths.shape, jnp.int32),
            pltpu.SMEM(rewards.shape, jnp.int32),
            pltpu.VMEM((tokens, ff), bf16),
            pltpu.VMEM((tokens, width), bf16),
            pltpu.VMEM((rank, width), bf16),
            pltpu.VMEM((ff, rank), bf16),
            pltpu.VMEM((ff, rank), bf16),
            pltpu.VMEM((2 * depth, rows, rank), bf16),
            pltpu.VMEM((depth, rows, rank), bf16),
            pltpu.VMEM((depth, rows, rank), bf16),
            pltpu.VMEM((2, tokens, rank), f32),
            pltpu.VMEM((2, tokens, rank), f32),
            pltpu.VMEM((tokens, rank), f32),
            pltpu.VMEM((tokens, rank), bf16),
            pltpu.VMEM((rank, width), f32),
            pltpu.VMEM((rank, width), bf16),
            pltpu.VMEM((rank // 2, width), bf16),
            pltpu.VMEM((quarter, width), bf16),
            pltpu.VMEM((quarter, width), bf16),
            pltpu.VMEM((quarter, width), bf16),
            pltpu.VMEM((depth, quarter, chunk), bf16),
            pltpu.VMEM((rank, width), bf16),
            pltpu.VMEM((2, 8, 128), f32),
            pltpu.VMEM((8, 128), f32),
            pltpu.VMEM((8, 128), f32),
            pltpu.VMEM((depth, 8, 128), f32),
            dma((7,)), dma((n - 1 + 0,)), dma((n,)),
            dma((2 * depth,)), dma((2 * depth,)),
            dma((depth,)), dma((depth,)), dma((depth,)), dma((depth,)),
            dma((2,)), dma((2,)),
            dma((4,)), dma((4,)), dma((depth,)), dma((depth,)), dma((depth,)), dma((depth,)),
            dma((2,)), dma((2,)), dma((depth,)), dma((depth,)),
        ],
        compiler_params=pltpu.CompilerParams(
            collective_id=0, has_side_effects=True, vmem_limit_bytes=48 * 1024 * 1024
        ),
        name="fused",
    )(
        *(
            pltpu.with_memory_space_constraint(v, pltpu.HBM)
            for v in (
                activations, output_gradient, adapter_a[0], adapter_b,
                log_ratio.reshape(-1, 128), lengths, rewards,
            )
        )
    )
    grad_a, grad_b, loss = pl.pallas_call(
        finish_kernel,
        out_shape=(
            jax.ShapeDtypeStruct((rows, rank), f32),
            jax.ShapeDtypeStruct((rank, width), f32),
            jax.ShapeDtypeStruct((1, 1), f32),
        ),
        in_specs=[vmem, vmem, vmem],
        out_specs=(hbm, hbm, scalars),
        scratch_shapes=[dma((2,))],
        compiler_params=pltpu.CompilerParams(vmem_limit_bytes=4 * 1024 * 1024),
        name="finish",
    )(grad_a, grad_b, loss)
    return grad_a[None], grad_b, loss.reshape(())


def fits(mesh):
    n, split = mesh.shape["dp"], mesh.shape["tensor"]
    return n % 4 == 0 and 4 <= n <= 16 and split == 2


def local(activations, output_gradient, adapter_a, adapter_b, log_ratio, lengths, rewards):
    n = lax.axis_size("dp")
    rows, rank = adapter_a.shape[1:]
    width, ff = output_gradient.shape[1], activations.shape[1]
    small = 2 * activations.size + 8 * ff * rank < 32 * 1024 * 1024
    aligned = (
        rows % 16 == 0
        and rank == 128
        and activations.shape[0] % 128 == 0
        and ff % 128 == 0
        and width % (128 * (n // 4)) == 0
        and n % lengths.shape[0] == 0
    )
    run = fused_local if small and aligned else plain_local
    return run(activations, output_gradient, adapter_a, adapter_b, log_ratio, lengths, rewards)


def solution(mesh):
    in_specs = (
        P("dp", "tensor"),
        P("dp", "tensor"),
        P("tensor", "dp", None),
        P(None, "tensor"),
        P("dp"),
        P(),
        P(),
    )
    out_specs = (P("tensor", "dp", None), P(None, "tensor"), P())
    body = local if fits(mesh) else plain_local
    return jax.shard_map(body, mesh=mesh, in_specs=in_specs, out_specs=out_specs, check_vma=False)
```

```python
import contextlib
import functools

import jax
import jax.numpy as jnp
from jax import lax
from jax.experimental import pallas as pl
from jax.experimental.pallas import tpu as pltpu
from jax.sharding import PartitionSpec as P

clip_eps = 0.2
adapter_scale_factor = 2.0


def token_terms(length_row, reward_row, log_ratio, offset):
    reward = reward_row.astype(jnp.float32)
    center = jnp.mean(reward)
    spread = jnp.mean((reward - center) * (reward - center))
    advantage = (reward - center) / jnp.sqrt(spread + 1.0)
    ends = jnp.cumsum(length_row)
    starts = ends - length_row
    slots = jnp.arange(log_ratio.shape[0], dtype=jnp.int32) + offset
    member = ((slots[None, :] >= starts[:, None]) & (slots[None, :] < ends[:, None])).astype(
        jnp.float32
    )
    live = jnp.sum(member, axis=0)
    token_adv = jnp.sum(member * advantage[:, None], axis=0)
    ratio = jnp.exp(log_ratio)
    unclipped = ratio * token_adv
    clipped = jnp.clip(ratio, 1.0 - clip_eps, 1.0 + clip_eps) * token_adv
    token_loss = -jnp.minimum(unclipped, clipped)
    slope = jnp.where(unclipped <= clipped, -unclipped, jnp.zeros_like(unclipped))
    return (live * slope, jnp.sum(live * token_loss), jnp.sum(live))


def plain_local(activations, output_gradient, adapter_a, adapter_b, log_ratio, lengths, rewards):
    tokens = activations.shape[0]
    groups = lengths.shape[0]
    per_group = lax.axis_size("dp") // groups
    position = lax.axis_index("dp")
    group_id = position // per_group
    offset = position % per_group * tokens
    length_row = lax.dynamic_index_in_dim(lengths, group_id, 0, keepdims=False)
    reward_row = lax.dynamic_index_in_dim(rewards, group_id, 0, keepdims=False)
    token_coefficient, loss_local, live_count = token_terms(
        length_row, reward_row, log_ratio, offset
    )
    columns = activations
    partial_low = jnp.dot(
        columns,
        lax.all_gather(adapter_a, "dp", axis=1, tiled=True)[0],
        preferred_element_type=jnp.float32,
    )
    partial_back = lax.dot_general(
        output_gradient, adapter_b, (((1,), (1,)), ((), ())), preferred_element_type=jnp.float32
    )
    low_rank, backward_projection = lax.psum((partial_low, partial_back), "tensor")
    error_rows = (adapter_scale_factor * token_coefficient[:, None] * backward_projection).astype(
        jnp.bfloat16
    )
    weighted_error = token_coefficient[:, None] * low_rank
    local_adapter_b_gradient = adapter_scale_factor * jnp.einsum(
        "tr,td->rd",
        weighted_error,
        output_gradient.astype(jnp.float32),
        precision=lax.Precision.HIGHEST,
    )
    columns = activations
    grad_a = lax.psum_scatter(
        lax.dot_general(
            columns, error_rows, (((0,), (0,)), ((), ())), preferred_element_type=jnp.float32
        ),
        "dp",
        scatter_dimension=0,
        tiled=True,
    )
    grad_b_sum, loss_sum, live_sum = lax.psum(
        (local_adapter_b_gradient, loss_local, live_count), "dp"
    )
    factor = groups / live_sum
    return ((factor * grad_a)[None], factor * grad_b_sum, factor * loss_sum)


MESH = pl.DeviceIdType.MESH
f32, bf16 = jnp.float32, jnp.bfloat16


def tile_of(total, most):
    return max(k for k in range(128, most + 1, 128) if total % k == 0)


SCOPES = False


def fused_kernel(
    n, groups, rollouts, cut_g, cut_r,
    act_hbm, grad_hbm, a_hbm, b_hbm, ratio_hbm, len_hbm, rew_hbm,
    out_a, out_b, out_loss,
    ratio_ref, len_ref, rew_ref,
    act, grad, b_mat, a_all, part, rs1, rs2, rs3, rs3x, rs4, xs, xr, coef, err,
    gb, gbs, gb1, gb2s, gb2, gb3s, gb3, fin, ls, l1, l2, lz,
    loc, send_s, ag_r, rs1_r, rs2_r, rs3_r, rs3x_r, rs4_r,
    x_r, g1_r, g2_r, g3_r, fin_r, l_r, lz_r,
):
    depth = n // 4
    last = depth - 1
    p = lax.axis_index("dp")
    t = lax.axis_index("tensor")
    c, y, z = p % 2, (p // 2) % 2, p // 4
    tokens, ff = act.shape
    rows, rank = a_hbm.shape
    width = grad.shape[1]
    half, quarter, chunk = rank // 2, rank // 4, width // depth

    def at(zz, yy, cc):
        return (zz * 2 + yy) * 2 + cc

    def remote(s, d, ss, rs, dev, tensor=None):
        return pltpu.make_async_remote_copy(
            src_ref=s, dst_ref=d, send_sem=ss, recv_sem=rs,
            device_id=(dev, t if tensor is None else tensor), device_id_type=MESH,
        )

    core, side = at(z, y, 1 - c), at(z, 1 - y, c)

    load_a = pltpu.make_async_copy(a_hbm, a_all.at[pl.ds(pl.multiple_of(p * rows, 16), rows)], loc.at[0])
    load_g = pltpu.make_async_copy(grad_hbm, grad, loc.at[1])
    load_b = pltpu.make_async_copy(b_hbm, b_mat, loc.at[2])
    load_x = pltpu.make_async_copy(act_hbm, act, loc.at[3])
    small = [
        pltpu.make_async_copy(s, d, loc.at[4 + i])
        for i, (s, d) in enumerate(((ratio_hbm, ratio_ref), (len_hbm, len_ref), (rew_hbm, rew_ref)))
    ]
    barrier = pltpu.get_barrier_semaphore()
    for dev in [core, side] + [at((z + k) % depth, y, c) for k in range(1, depth)]:
        pl.semaphore_signal(barrier, inc=1, device_id=(dev, t), device_id_type=MESH)
    pl.semaphore_signal(barrier, inc=1, device_id=(p, 1 - t), device_id_type=MESH)
    for copy in [load_a, load_g, load_b] + small + [load_x]:
        copy.start()
    load_g.wait()
    load_b.wait()
    xs[0] = lax.dot_general(grad[...], b_mat[...], (((1,), (1,)), ((), ())), preferred_element_type=f32)
    for copy in small:
        copy.wait()

    per_group = n // groups
    group = p // per_group
    offset = (p % per_group) * tokens
    slots = (
        lax.broadcasted_iota(jnp.int32, ratio_ref.shape, 0) * 128
        + lax.broadcasted_iota(jnp.int32, ratio_ref.shape, 1)
        + offset
    )
    live_total = jnp.int32(0)
    live = jnp.zeros(ratio_ref.shape, f32)
    token_adv = jnp.zeros(ratio_ref.shape, f32)
    for g in range(groups):
        here = jnp.full((1, 128), (group == g).astype(f32))
        reward = [jnp.full((1, 128), rew_ref[g, i]).astype(f32) for i in range(rollouts)]
        center = sum(reward) / rollouts
        spread = sum((r - center) * (r - center) for r in reward) / rollouts
        scale = jnp.sqrt(spread + 1.0)
        end = jnp.int32(0)
        for i in range(rollouts):
            start = end
            end = end + len_ref[g, i]
            member = ((slots >= start) & (slots < end)).astype(f32) * here
            live = live + member
            token_adv = token_adv + member * ((reward[i] - center) / scale)
        live_total = live_total + jnp.minimum(end, per_group * tokens)
    ratio = jnp.exp(ratio_ref[...])
    unclipped = ratio * token_adv
    clipped = jnp.clip(ratio, 1.0 - clip_eps, 1.0 + clip_eps) * token_adv
    token_loss = -jnp.minimum(unclipped, clipped)
    slope = jnp.where(unclipped <= clipped, -unclipped, jnp.zeros_like(unclipped))
    weight = live * slope
    for i in range(tokens // 128):
        coef[pl.ds(i * 128, 128), :] = jnp.broadcast_to(weight[i : i + 1, :], (128, 128)).T
    factor = groups / jnp.full((1, 128), live_total).astype(f32)
    loss_part = jnp.sum(jnp.sum(live * token_loss, axis=1, keepdims=True), axis=0, keepdims=True)
    ls[0] = jnp.broadcast_to(loss_part, (8, 128))
    load_a.wait()
    load_x.wait()
    with jax.named_scope("barrier") if SCOPES else contextlib.nullcontext():
        pl.semaphore_wait(barrier, depth + 2)

    flip = (2 * z > last).astype(jnp.int32)
    tile = tile_of(4 * rows, 1280)
    steps = 4 * rows // tile

    def run(u):
        sent = []

        def m(k):
            return k + flip * (last - 2 * k)

        def dev(k, yy, cc):
            return at(m(k), yy, cc)

        others = sorted((k for k in range(depth) if k != u), key=lambda k: abs(k - u))
        up = u + 1 if u < last else None
        down = u - 1 if u > 0 else None

        def onward(k):
            return up if k < u else down

        def go(s, d, rs, device, tensor=None):
            copy = remote(s, d, send_s.at[len(sent)], rs, device, tensor)
            copy.start()
            sent.append(copy)

        def got(d, rs):
            remote(d, d, send_s.at[0], rs, core).wait_recv()

        def z_dev(k):
            return dev(k, y, c)

        def piece(k, yy, cc, i):
            q = dev(k, yy, cc)
            low, size = (0, cut_g) if i == 0 else (cut_g, rows - cut_g)
            return a_all.at[pl.ds(pl.multiple_of(q * rows + low, 16), size)], ag_r.at[2 * q + i]

        def a_send(k, yy, i, *devices):
            ref, sem = piece(k, yy, c, i)
            for device in devices:
                if device is not None:
                    go(ref, ref, sem, device)

        def a_wait(k, yy, cc, i):
            got(*piece(k, yy, cc, i))

        up_dev = None if up is None else z_dev(up)
        down_dev = None if down is None else z_dev(down)

        def a_start():
            a_send(u, y, 0, up_dev, down_dev)
            a_send(u, y, 1, side, up_dev, down_dev)
            a_send(u, y, 0, side)
            a_send(u, y, 0, core)
            a_send(u, y, 1, core)

        def a_side(i):
            a_wait(u, 1 - y, c, i)
            if i == 1:
                a_send(u, 1 - y, 1, up_dev, down_dev)
            a_send(u, 1 - y, i, core)

        def a_line(k, yy, i):
            a_wait(k, yy, c, i)
            to = onward(k)
            a_send(k, yy, i, None if to is None else z_dev(to))
            if i == 0:
                a_send(k, yy, i, side)
            a_send(k, yy, i, core)

        def a_over(k):
            a_wait(k, 1 - y, c, 0)
            a_send(k, 1 - y, 0, core)

        def low_of(k, first):
            for yy in (0, 1):
                for i in (0, 1):
                    a_wait(k, yy, 1 - c, i)
            base = m(k) * (4 * rows)

            def step(i, total):
                cols = pl.ds(pl.multiple_of(base + i * tile, 128), tile)
                return total + jnp.dot(act[:, cols], a_all[cols, :], preferred_element_type=f32)

            begin = jnp.zeros((tokens, rank), f32) if first else xs[1]
            xs[1] = lax.fori_loop(0, steps, step, begin)

        def low_send():
            go(xs.at[1], xr.at[1], x_r.at[1], p, 1 - t)

        def loss_one():
            go(ls.at[0], l1, l_r.at[0], core)

        def loss_two():
            got(l1, l_r.at[0])
            ls[1] = ls[0] + l1[...]
            go(ls.at[1], l2, l_r.at[1], side)

        def loss_three():
            got(l2, l_r.at[1])
            lz[z] = ls[1] + l2[...]
            for k in others:
                go(lz.at[z], lz.at[z], lz_r.at[z], z_dev(k))

        def loss_end():
            for k in others:
                got(lz.at[m(k)], lz_r.at[m(k)])
            total = lz[0]
            for i in range(1, depth):
                total = total + lz[i]
            out_loss[...] = factor * total

        def back_send():
            go(xs.at[0], xr.at[0], x_r.at[0], p, 1 - t)

        def back_end():
            got(xr.at[0], x_r.at[0])
            err[...] = (adapter_scale_factor * coef[...] * (xs[0] + xr[0])).astype(bf16)

        def span(k, yy, cc, part_two=None):
            q = dev(k, yy, cc)
            low, size = {None: (0, rows), 0: (0, cut_r), 1: (cut_r, rows - cut_r)}[part_two]
            return part.at[pl.ds(pl.multiple_of(q * rows + low, 16), size)]

        def part_of(k):
            base = m(k) * (4 * rows)

            def step(i, _):
                cols = pl.ds(pl.multiple_of(base + i * tile, 128), tile)
                part[cols, :] = lax.dot_general(
                    act[:, cols], err[...], (((0,), (0,)), ((), ())), preferred_element_type=f32
                ).astype(bf16)
                return 0

            lax.fori_loop(0, steps, step, 0)
            for yy in (1 - y, y):
                slot = m(k) * 2 + yy
                go(span(k, yy, 1 - c), rs1.at[slot], rs1_r.at[slot], core)

        def both(k, yy, i):
            low, size = (0, cut_r) if i == 0 else (cut_r, rows - cut_r)
            return span(k, yy, c, i)[...].astype(f32) + rs1[m(k) * 2 + yy, pl.ds(low, size), :].astype(f32)

        def core_sum(k):
            for yy in (1 - y, y):
                slot = m(k) * 2 + yy
                got(rs1.at[slot], rs1_r.at[slot])
            ref = span(k, 1 - y, c, 0)
            ref[...] = both(k, 1 - y, 0).astype(bf16)
            go(ref, rs2.at[m(k)], rs2_r.at[m(k)], side)

        def line_slot(k, upward):
            return (flip if upward else 1 - flip) * depth + m(k)

        def sources(k):
            found = []
            if k >= u and down is not None:
                found.append(line_slot(k, True))
            if k <= u and up is not None:
                found.append(line_slot(k, False))
            return found

        def line_x(k):
            total = both(k, 1 - y, 1)
            for slot in sources(k):
                got(rs3x.at[slot], rs3x_r.at[slot])
                total = total + rs3x[slot].astype(f32)
            ref = span(k, 1 - y, c, 1)
            ref[...] = total.astype(bf16)
            if k == u:
                go(ref, rs4, rs4_r.at[0], side)
            else:
                slot = line_slot(k, k > u)
                go(ref, rs3x.at[slot], rs3x_r.at[slot], z_dev(up if k > u else down))

        def line_sum(k):
            slots_in = sources(k)
            got(rs2.at[m(k)], rs2_r.at[m(k)])
            for slot in slots_in:
                got(rs3.at[slot], rs3_r.at[slot])
            first = both(k, y, 0) + rs2[m(k)].astype(f32)
            second = both(k, y, 1)
            for slot in slots_in:
                first = first + rs3[slot, pl.ds(0, cut_r), :].astype(f32)
                second = second + rs3[slot, pl.ds(cut_r, rows - cut_r), :].astype(f32)
            if k == u:
                out_a[pl.ds(0, cut_r), :] = factor * first
                out_a[pl.ds(cut_r, rows - cut_r), :] = second
            else:
                ref = span(k, y, c, 0)
                ref[...] = first.astype(bf16)
                ref = span(k, y, c, 1)
                ref[...] = second.astype(bf16)
                slot = line_slot(k, k > u)
                go(span(k, y, c), rs3.at[slot], rs3_r.at[slot], z_dev(up if k > u else down))

        def a_end():
            got(rs4, rs4_r.at[0])
            rest = pl.ds(cut_r, rows - cut_r)
            out_a[rest, :] = factor * (out_a[rest, :] + rs4[...].astype(f32))

        lane = pl.multiple_of(c * half, 16)
        other = pl.multiple_of((1 - c) * half, 16)
        away = pl.multiple_of((1 - y) * quarter, 16)
        stay = pl.multiple_of(y * quarter, 16)
        mine = pl.multiple_of(lane + stay, 16)
        b_order = others[::-1] + [u]

        def cols_of(k):
            return pl.ds(pl.multiple_of(m(k) * chunk, 128), chunk)

        def b_part():
            got(xr.at[1], x_r.at[1])
            weighted = coef[...] * (xs[1] + xr[1])
            high = weighted.astype(bf16)
            rest = weighted - high.astype(f32)
            middle = rest.astype(bf16)
            last_part = (rest - middle.astype(f32)).astype(bf16)
            for k in b_order:
                cols = cols_of(k)
                total = sum(
                    lax.dot_general(w, grad[:, cols], (((0,), (0,)), ((), ())), preferred_element_type=f32)
                    for w in (last_part, middle, high)
                )
                gb[:, cols] = total
                gbs[:, cols] = total.astype(bf16)
                go(gbs.at[pl.ds(other, half), cols], gb1.at[:, cols], g1_r.at[m(k)], core)

        def b_core(k):
            cols = cols_of(k)
            got(gb1.at[:, cols], g1_r.at[m(k)])
            gb2s[:, cols] = (
                gb[pl.ds(pl.multiple_of(lane + away, 16), quarter), cols]
                + gb1[pl.ds(away, quarter), cols].astype(f32)
            ).astype(bf16)
            go(gb2s.at[:, cols], gb2.at[:, cols], g2_r.at[m(k)], side)

        def b_side(k):
            cols = cols_of(k)
            got(gb2.at[:, cols], g2_r.at[m(k)])
            total = (
                gb[pl.ds(mine, quarter), cols]
                + gb1[pl.ds(stay, quarter), cols].astype(f32)
                + gb2[:, cols].astype(f32)
            )
            if k == u:
                gb[pl.ds(mine, quarter), cols] = total
            else:
                gb3s[:, cols] = total.astype(bf16)
                go(gb3s.at[:, cols], gb3.at[z], g3_r.at[z], z_dev(k))

        def final(k, yy, cc):
            at_row = pl.multiple_of(cc * half + yy * quarter, 16)
            return fin.at[pl.ds(at_row, quarter), cols_of(k)], fin_r.at[dev(k, yy, cc)]

        def b_send(k, yy, *devices):
            ref, sem = final(k, yy, c)
            for device in devices:
                go(ref, ref, sem, device)

        def b_line():
            cols = cols_of(u)
            total = gb[pl.ds(mine, quarter), cols]
            for k in others:
                got(gb3.at[m(k)], g3_r.at[m(k)])
                total = total + gb3[m(k)].astype(f32)
            scaled = jnp.full((1, 128), adapter_scale_factor) * factor
            fin[pl.ds(mine, quarter), cols] = (scaled[:, :1] * total).astype(bf16)
            b_send(u, y, *[z_dev(k) for k in others[::-1]], side, core)

        def b_pass(k, yy):
            got(*final(k, yy, c))
            if yy is y:
                b_send(k, yy, side)
            b_send(k, yy, core)

        def b_end():
            for k in [u] + others:
                for yy in (y, 1 - y):
                    got(*final(k, yy, 1 - c))
            out_b[...] = fin[...].astype(f32)

        there = 1 - y
        plan = [
            (0.0, a_start), (0.1, back_send), (0.2, loss_one),
            (3.0, a_side, 1), (4.5, back_end), (6.4, a_side, 0), (7.2, loss_two), (9.5, loss_three),
        ]
        order = [k for k in (range(last, -1, -1)) if k > u] + [k for k in range(u)] + [u]
        for i, k in enumerate(order):
            plan.append((4.6 + 0.95 * i, part_of, k))
            plan.append((7.05 + 0.95 * i, core_sum, k))
        if u == 0:
            for i, k in enumerate(order[:-1]):
                plan.append(((7.1, 8.1, 12.0)[i % 3], line_x, k))
                plan.append(((11.0, 13.0, 14.0)[i % 3], line_sum, k))
            plan.append((22.0, line_x, u))
            plan.append((30.0, line_sum, u))
        else:
            for k in order:
                if k > u:
                    plan.append((11.5 + 2.0 * (last - k), line_x, k))
                    plan.append((17.0 + 5.0 * (last - k), line_sum, k))
                elif k < u:
                    plan.append((16.0, line_x, k))
                    plan.append((23.5, line_sum, k))
                else:
                    plan.append((20.0, line_x, k))
                    plan.append((30.0, line_sum, k))
        plan.append((31.0, a_end))
        when = {}
        for k in others:
            hops = abs(k - u)
            when[k] = 5.2 + 6.0 * (hops - 1)
            plan.append((when[k], a_line, k, y, 0))
            plan.append((when[k] + 1.2, a_line, k, y, 1))
            plan.append((when[k] + 2.5, a_line, k, there, 1))
            plan.append((when[k] + 5.2, a_over, k))
        for i, k in enumerate([u] + others):
            done = 9.0 if i == 0 else when[k] + 6.4 + 0.1 * i
            plan.append((done, low_of, k, i == 0))
        plan.append((done + 0.1, low_send))
        begin = done + 5.0
        plan.append((begin, b_part))
        for i, k in enumerate(b_order):
            plan.append((begin + 1.5 + 0.01 * i, b_core, k))
            plan.append((begin + 4.5 + 0.9 * i, b_side, k))
        begin = 6.0 * last + 10.6 + 0.1 * last
        plan.append((begin + 9.5, b_line))
        plan.append((begin + 11.5, b_pass, u, there))
        for i, k in enumerate(others):
            plan.append((begin + 12.0 + 0.9 * i, b_pass, k, y))
            plan.append((begin + 14.0 + 0.9 * i, b_pass, k, there))
        plan.append((begin + 18.0, loss_end))
        plan.append((begin + 19.0, b_end))
        for entry in sorted(plan, key=lambda e: e[0]):
            name = entry[1].__name__ + "_".join(str(v) for v in entry[2:] if isinstance(v, int))
            with jax.named_scope(name) if SCOPES else contextlib.nullcontext():
                entry[1](*entry[2:])
        for copy in sent:
            copy.wait_send()

    for u in range((depth + 1) // 2):
        @pl.when(jnp.minimum(z, last - z) == u)
        def _():
            run(u)


def finish_kernel(a_in, b_in, loss_in, a_out, b_out, loss_out, sems):
    copies = [
        pltpu.make_async_copy(s, d, sems.at[i])
        for i, (s, d) in enumerate(((a_in, a_out), (b_in, b_out)))
    ]
    for copy in copies:
        copy.start()
    loss_out[0, 0] = loss_in[0, 0]
    for copy in copies:
        copy.wait()


def fused_local(activations, output_gradient, adapter_a, adapter_b, log_ratio, lengths, rewards):
    n = lax.axis_size("dp")
    depth = n // 4
    tokens, ff = activations.shape
    rows, rank = adapter_a.shape[1:]
    width = output_gradient.shape[1]
    dma = pltpu.SemaphoreType.DMA
    vmem, anywhere = pl.BlockSpec(memory_space=pltpu.VMEM), pl.BlockSpec(memory_space=pl.ANY)
    scalars = pl.BlockSpec(memory_space=pltpu.SMEM)
    hbm = pl.BlockSpec(memory_space=pltpu.HBM)
    quarter, chunk = rank // 4, width // depth
    cut_g, cut_r = rows * 3 // 64 * 16, rows // 32 * 16
    grad_a, grad_b, loss = pl.pallas_call(
        functools.partial(fused_kernel, n, lengths.shape[0], lengths.shape[1], cut_g, cut_r),
        out_shape=(
            jax.ShapeDtypeStruct((rows, rank), f32),
            jax.ShapeDtypeStruct((rank, width), f32),
            jax.ShapeDtypeStruct((8, 128), f32),
        ),
        in_specs=[hbm] * 7,
        out_specs=(vmem, vmem, vmem),
        scratch_shapes=[
            pltpu.VMEM((tokens // 128, 128), f32),
            pltpu.SMEM(lengths.shape, jnp.int32),
            pltpu.SMEM(rewards.shape, jnp.int32),
            pltpu.VMEM((tokens, ff), bf16),
            pltpu.VMEM((tokens, width), bf16),
            pltpu.VMEM((rank, width), bf16),
            pltpu.VMEM((ff, rank), bf16),
            pltpu.VMEM((ff, rank), bf16),
            pltpu.VMEM((2 * depth, rows, rank), bf16),
            pltpu.VMEM((depth, cut_r, rank), bf16),
            pltpu.VMEM((2 * depth, rows, rank), bf16),
            pltpu.VMEM((2 * depth, rows - cut_r, rank), bf16),
            pltpu.VMEM((rows - cut_r, rank), bf16),
            pltpu.VMEM((2, tokens, rank), f32),
            pltpu.VMEM((2, tokens, rank), f32),
            pltpu.VMEM((tokens, rank), f32),
            pltpu.VMEM((tokens, rank), bf16),
            pltpu.VMEM((rank, width), f32),
            pltpu.VMEM((rank, width), bf16),
            pltpu.VMEM((rank // 2, width), bf16),
            pltpu.VMEM((quarter, width), bf16),
            pltpu.VMEM((quarter, width), bf16),
            pltpu.VMEM((quarter, width), bf16),
            pltpu.VMEM((depth, quarter, chunk), bf16),
            pltpu.VMEM((rank, width), bf16),
            pltpu.VMEM((2, 8, 128), f32),
            pltpu.VMEM((8, 128), f32),
            pltpu.VMEM((8, 128), f32),
            pltpu.VMEM((depth, 8, 128), f32),
            dma((7,)), dma((144,)), dma((2 * n,)),
            dma((2 * depth,)), dma((depth,)), dma((2 * depth,)), dma((2 * depth,)), dma((1,)),
            dma((2,)), dma((depth,)), dma((depth,)), dma((depth,)), dma((n,)),
            dma((2,)), dma((depth,)),
        ],
        compiler_params=pltpu.CompilerParams(
            collective_id=0, has_side_effects=True, vmem_limit_bytes=48 * 1024 * 1024
        ),
        name="fused",
    )(
        *(
            pltpu.with_memory_space_constraint(v, pltpu.HBM)
            for v in (
                activations, output_gradient, adapter_a[0], adapter_b,
                log_ratio.reshape(-1, 128), lengths, rewards,
            )
        )
    )
    grad_a, grad_b, loss = pl.pallas_call(
        finish_kernel,
        out_shape=(
            jax.ShapeDtypeStruct((rows, rank), f32),
            jax.ShapeDtypeStruct((rank, width), f32),
            jax.ShapeDtypeStruct((1, 1), f32),
        ),
        in_specs=[vmem, vmem, vmem],
        out_specs=(hbm, hbm, scalars),
        scratch_shapes=[dma((2,))],
        compiler_params=pltpu.CompilerParams(vmem_limit_bytes=4 * 1024 * 1024),
        name="finish",
    )(grad_a, grad_b, loss)
    return grad_a[None], grad_b, loss.reshape(())


def fits(mesh):
    n, split = mesh.shape["dp"], mesh.shape["tensor"]
    return n % 4 == 0 and 4 <= n <= 16 and split == 2


def local(activations, output_gradient, adapter_a, adapter_b, log_ratio, lengths, rewards):
    n = lax.axis_size("dp")
    rows, rank = adapter_a.shape[1:]
    width, ff = output_gradient.shape[1], activations.shape[1]
    small = 2 * activations.size + 8 * ff * rank < 32 * 1024 * 1024
    aligned = (
        rows % 16 == 0
        and rank == 128
        and activations.shape[0] % 128 == 0
        and ff % 128 == 0
        and 4 * rows % 128 == 0
        and rows >= 64
        and width % (128 * (n // 4)) == 0
        and n % lengths.shape[0] == 0
    )
    run = fused_local if small and aligned else plain_local
    return run(activations, output_gradient, adapter_a, adapter_b, log_ratio, lengths, rewards)


def solution(mesh):
    in_specs = (
        P("dp", "tensor"),
        P("dp", "tensor"),
        P("tensor", "dp", None),
        P(None, "tensor"),
        P("dp"),
        P(),
        P(),
    )
    out_specs = (P("tensor", "dp", None), P(None, "tensor"), P())
    body = local if fits(mesh) else plain_local
    return jax.shard_map(body, mesh=mesh, in_specs=in_specs, out_specs=out_specs, check_vma=False)
```

```python
import contextlib
import functools
import math

import jax
import jax.numpy as jnp
from jax import lax
from jax.experimental import pallas as pl
from jax.experimental.pallas import tpu as pltpu
from jax.sharding import PartitionSpec as P

clip_eps = 0.2
adapter_scale_factor = 2.0


def token_terms(length_row, reward_row, log_ratio, offset):
    reward = reward_row.astype(jnp.float32)
    center = jnp.mean(reward)
    spread = jnp.mean((reward - center) * (reward - center))
    advantage = (reward - center) / jnp.sqrt(spread + 1.0)
    ends = jnp.cumsum(length_row)
    starts = ends - length_row
    slots = jnp.arange(log_ratio.shape[0], dtype=jnp.int32) + offset
    member = ((slots[None, :] >= starts[:, None]) & (slots[None, :] < ends[:, None])).astype(
        jnp.float32
    )
    live = jnp.sum(member, axis=0)
    token_adv = jnp.sum(member * advantage[:, None], axis=0)
    ratio = jnp.exp(log_ratio)
    unclipped = ratio * token_adv
    clipped = jnp.clip(ratio, 1.0 - clip_eps, 1.0 + clip_eps) * token_adv
    token_loss = -jnp.minimum(unclipped, clipped)
    slope = jnp.where(unclipped <= clipped, -unclipped, jnp.zeros_like(unclipped))
    return (live * slope, jnp.sum(live * token_loss), jnp.sum(live))


def plain_local(activations, output_gradient, adapter_a, adapter_b, log_ratio, lengths, rewards):
    tokens = activations.shape[0]
    groups = lengths.shape[0]
    per_group = lax.axis_size("dp") // groups
    position = lax.axis_index("dp")
    group_id = position // per_group
    offset = position % per_group * tokens
    length_row = lax.dynamic_index_in_dim(lengths, group_id, 0, keepdims=False)
    reward_row = lax.dynamic_index_in_dim(rewards, group_id, 0, keepdims=False)
    token_coefficient, loss_local, live_count = token_terms(
        length_row, reward_row, log_ratio, offset
    )
    columns = activations
    partial_low = jnp.dot(
        columns,
        lax.all_gather(adapter_a, "dp", axis=1, tiled=True)[0],
        preferred_element_type=jnp.float32,
    )
    partial_back = lax.dot_general(
        output_gradient, adapter_b, (((1,), (1,)), ((), ())), preferred_element_type=jnp.float32
    )
    low_rank, backward_projection = lax.psum((partial_low, partial_back), "tensor")
    error_rows = (adapter_scale_factor * token_coefficient[:, None] * backward_projection).astype(
        jnp.bfloat16
    )
    weighted_error = token_coefficient[:, None] * low_rank
    local_adapter_b_gradient = adapter_scale_factor * jnp.einsum(
        "tr,td->rd",
        weighted_error,
        output_gradient.astype(jnp.float32),
        precision=lax.Precision.HIGHEST,
    )
    columns = activations
    grad_a = lax.psum_scatter(
        lax.dot_general(
            columns, error_rows, (((0,), (0,)), ((), ())), preferred_element_type=jnp.float32
        ),
        "dp",
        scatter_dimension=0,
        tiled=True,
    )
    grad_b_sum, loss_sum, live_sum = lax.psum(
        (local_adapter_b_gradient, loss_local, live_count), "dp"
    )
    factor = groups / live_sum
    return ((factor * grad_a)[None], factor * grad_b_sum, factor * loss_sum)


MESH = pl.DeviceIdType.MESH
f32, bf16 = jnp.float32, jnp.bfloat16


def tile_of(total, most):
    return max(k for k in range(128, most + 1, 128) if total % k == 0)


SCOPES = False


def fused_kernel(
    n, groups, rollouts, cut_g, cut_r,
    act_hbm, grad_hbm, a_hbm, b_hbm, ratio_hbm, len_hbm, rew_hbm,
    out_a, out_b, out_loss,
    ratio_ref, len_ref, rew_ref,
    act, grad, b_mat, a_all, part, rs1, rs2, rs3, rs3x, rs4, xs, xr, low_s, low_r, coef, err,
    gb, gbs, gb1, gb2s, gb2, gb3s, gb3, fin, ls, l1, l2, lz,
    fac, loc, send_s, ag_r, ag_c, rs1_r, rs2_r, rs3_r, rs3x_r, rs4_r,
    x_r, g1_r, g2_r, g3_r, fin_r, l_r, lz_r,
):
    depth = n // 4
    last = depth - 1
    p = lax.axis_index("dp")
    t = lax.axis_index("tensor")
    c, y, z = p % 2, (p // 2) % 2, p // 4
    tokens, ff = act.shape
    rows, rank = a_hbm.shape
    width = grad.shape[1]
    half, quarter, chunk = rank // 2, rank // 4, width // depth

    def at(zz, yy, cc):
        return (zz * 2 + yy) * 2 + cc

    def remote(s, d, ss, rs, dev, tensor=None):
        return pltpu.make_async_remote_copy(
            src_ref=s, dst_ref=d, send_sem=ss, recv_sem=rs,
            device_id=(dev, t if tensor is None else tensor), device_id_type=MESH,
        )

    core, side = at(z, y, 1 - c), at(z, 1 - y, c)

    load_a = pltpu.make_async_copy(a_hbm, a_all.at[pl.ds(pl.multiple_of(p * rows, 16), rows)], loc.at[0])
    load_g = pltpu.make_async_copy(grad_hbm, grad, loc.at[1])
    load_b = pltpu.make_async_copy(b_hbm, b_mat, loc.at[2])
    load_x = pltpu.make_async_copy(act_hbm, act, loc.at[3])
    small = [
        pltpu.make_async_copy(s, d, loc.at[4 + i])
        for i, (s, d) in enumerate(((ratio_hbm, ratio_ref), (len_hbm, len_ref), (rew_hbm, rew_ref)))
    ]
    barrier = pltpu.get_barrier_semaphore()
    for dev in [core, side] + [at((z + k) % depth, y, c) for k in range(1, depth)]:
        pl.semaphore_signal(barrier, inc=1, device_id=(dev, t), device_id_type=MESH)
    pl.semaphore_signal(barrier, inc=1, device_id=(p, 1 - t), device_id_type=MESH)
    for copy in [load_a, load_g, load_b] + small + [load_x]:
        copy.start()
    load_a.wait()
    with jax.named_scope("barrier") if SCOPES else contextlib.nullcontext():
        pl.semaphore_wait(barrier, depth + 2)
    flip = (2 * z > last).astype(jnp.int32)
    tile = tile_of(4 * rows, 1280)
    steps = 4 * rows // tile

    def run(u):
        sent = []

        def m(k):
            return k + flip * (last - 2 * k)

        def dev(k, yy, cc):
            return at(m(k), yy, cc)

        others = sorted((k for k in range(depth) if k != u), key=lambda k: abs(k - u))
        up = u + 1 if u < last else None
        down = u - 1 if u > 0 else None

        def onward(k):
            return up if k < u else down

        def go(s, d, rs, device, tensor=None):
            size = s.dtype.itemsize * math.prod(s.shape) // 256
            if not sent or sent[-1] + size > ff:
                sent.append(0)
            sent[-1] += size
            remote(s, d, send_s.at[len(sent) - 1], rs, device, tensor).start()

        def drain():
            for i, size in enumerate(sent):
                ref = a_all.at[pl.ds(0, size)]
                remote(ref, ref, send_s.at[i], send_s.at[i], core).wait_send()

        def got(d, rs):
            remote(d, d, send_s.at[0], rs, core).wait_recv()

        def z_dev(k):
            return dev(k, y, c)

        cuts = [(0, cut_g // 32 * 16), (cut_g // 32 * 16, cut_g), (cut_g, rows)]

        def piece(k, yy, i):
            low, high = cuts[i]
            ref = a_all.at[pl.ds(pl.multiple_of(dev(k, yy, c) * rows + low, 16), high - low)]
            return ref, ag_r.at[(m(k) * 2 + yy) * 3 + i]

        def a_send(k, yy, i, *devices):
            ref, sem = piece(k, yy, i)
            for device in devices:
                if device is not None:
                    go(ref, ref, sem if device is not core else ag_c.at[m(k) * 2 + yy], device)

        def a_wait(k, yy, i):
            got(*piece(k, yy, i))

        def a_core(k, yy):
            got(
                a_all.at[pl.ds(pl.multiple_of(dev(k, yy, 1 - c) * rows, 16), rows)],
                ag_c.at[m(k) * 2 + yy],
            )

        up_dev = None if up is None else z_dev(up)
        down_dev = None if down is None else z_dev(down)

        def a_start():
            a_send(u, y, 0, up_dev, down_dev)
            a_send(u, y, 2, side)
            a_send(u, y, 1, up_dev, down_dev)
            a_send(u, y, 2, up_dev, down_dev)
            a_send(u, y, 0, side)
            a_send(u, y, 1, side)
            for i in range(3):
                a_send(u, y, i, core)

        def a_side(i):
            a_wait(u, 1 - y, i)
            if i == 2:
                a_send(u, 1 - y, i, up_dev, down_dev)
            a_send(u, 1 - y, i, core)

        def a_line(k, yy, i):
            a_wait(k, yy, i)
            to = onward(k)
            a_send(k, yy, i, None if to is None else z_dev(to))
            if i < 2:
                a_send(k, yy, i, side)
            a_send(k, yy, i, core)

        def a_over(k, i):
            a_wait(k, 1 - y, i)
            a_send(k, 1 - y, i, core)

        def low_rows(start, size, first=False):
            width_of = size if size <= 2048 else tile_of(size, 1280)

            def step(i, total):
                cols = pl.ds(pl.multiple_of(start + i * width_of, 128), width_of)
                return total + jnp.dot(act[:, cols], a_all[cols, :], preferred_element_type=f32)

            begin = jnp.zeros((tokens, rank), f32) if first else xs[1]
            xs[1] = lax.fori_loop(0, size // width_of, step, begin)

        def low_of(k, first):
            for yy in (0, 1):
                a_core(k, yy)
            low_rows(m(k) * (4 * rows), 4 * rows, first)

        small_part = 2 * rows // 128 * 128

        def low_near(k):
            a_core(k, y)
            low_rows(m(k) * (4 * rows) + y * (4 * rows - small_part), small_part)

        def low_far(k):
            a_core(k, 1 - y)
            low_rows(m(k) * (4 * rows) + (1 - y) * small_part, 4 * rows - small_part)

        def low_send():
            low_s[...] = xs[1].astype(bf16)
            go(low_s, low_r, x_r.at[1], p, 1 - t)

        def loss_one():
            go(ls.at[0], l1, l_r.at[0], core)

        def loss_two():
            got(l1, l_r.at[0])
            ls[1] = ls[0] + l1[...]
            go(ls.at[1], l2, l_r.at[1], side)

        def loss_three():
            got(l2, l_r.at[1])
            lz[z] = ls[1] + l2[...]
            for k in others:
                go(lz.at[z], lz.at[z], lz_r.at[z], z_dev(k))

        def loss_end():
            for k in others:
                got(lz.at[m(k)], lz_r.at[m(k)])
            total = lz[0]
            for i in range(1, depth):
                total = total + lz[i]
            out_loss[...] = fac[...] * total

        def back_send():
            load_g.wait()
            load_b.wait()
            xs[0] = lax.dot_general(
                grad[...], b_mat[...], (((1,), (1,)), ((), ())), preferred_element_type=f32
            )
            go(xs.at[0], xr, x_r.at[0], p, 1 - t)

        def token_terms_here():
            for copy in small:
                copy.wait()
            per_group = n // groups
            group = p // per_group
            offset = (p % per_group) * tokens
            slots = (
                lax.broadcasted_iota(jnp.int32, ratio_ref.shape, 0) * 128
                + lax.broadcasted_iota(jnp.int32, ratio_ref.shape, 1)
                + offset
            )
            live_total = jnp.int32(0)
            live = jnp.zeros(ratio_ref.shape, f32)
            token_adv = jnp.zeros(ratio_ref.shape, f32)
            for g in range(groups):
                here = jnp.full((1, 128), (group == g).astype(f32))
                reward = [jnp.full((1, 128), rew_ref[g, i]).astype(f32) for i in range(rollouts)]
                center = sum(reward) / rollouts
                spread = sum((r - center) * (r - center) for r in reward) / rollouts
                scale = jnp.sqrt(spread + 1.0)
                end = jnp.int32(0)
                for i in range(rollouts):
                    start = end
                    end = end + len_ref[g, i]
                    member = ((slots >= start) & (slots < end)).astype(f32) * here
                    live = live + member
                    token_adv = token_adv + member * ((reward[i] - center) / scale)
                live_total = live_total + jnp.minimum(end, per_group * tokens)
            ratio = jnp.exp(ratio_ref[...])
            unclipped = ratio * token_adv
            clipped = jnp.clip(ratio, 1.0 - clip_eps, 1.0 + clip_eps) * token_adv
            token_loss = -jnp.minimum(unclipped, clipped)
            slope = jnp.where(unclipped <= clipped, -unclipped, jnp.zeros_like(unclipped))
            weight = live * slope
            for i in range(tokens // 128):
                coef[pl.ds(i * 128, 128), :] = jnp.broadcast_to(weight[i : i + 1, :], (128, 128)).T
            fac[...] = groups / jnp.full((1, 128), live_total).astype(f32)
            loss_part = jnp.sum(jnp.sum(live * token_loss, axis=1, keepdims=True), axis=0, keepdims=True)
            ls[0] = jnp.broadcast_to(loss_part, (8, 128))

        def back_end():
            got(xr, x_r.at[0])
            err[...] = (adapter_scale_factor * coef[...] * (xs[0] + xr[...])).astype(bf16)

        def span(k, yy, cc, part_two=None):
            q = dev(k, yy, cc)
            low, size = {None: (0, rows), 0: (0, cut_r), 1: (cut_r, rows - cut_r)}[part_two]
            return part.at[pl.ds(pl.multiple_of(q * rows + low, 16), size)]

        def part_of(k):
            base = m(k) * (4 * rows)

            def step(i, _):
                cols = pl.ds(pl.multiple_of(base + i * tile, 128), tile)
                part[cols, :] = lax.dot_general(
                    act[:, cols], err[...], (((0,), (0,)), ((), ())), preferred_element_type=f32
                ).astype(bf16)
                return 0

            lax.fori_loop(0, steps, step, 0)
            for yy in (1 - y, y):
                slot = m(k) * 2 + yy
                go(span(k, yy, 1 - c), rs1.at[slot], rs1_r.at[m(k)], core)

        def both(k, yy, i):
            low, size = (0, cut_r) if i == 0 else (cut_r, rows - cut_r)
            return span(k, yy, c, i)[...].astype(f32) + rs1[m(k) * 2 + yy, pl.ds(low, size), :].astype(f32)

        def core_wait(k):
            got(rs1.at[pl.ds(m(k) * 2, 2)], rs1_r.at[m(k)])

        def core_sum(k):
            ref = span(k, 1 - y, c, 0)
            ref[...] = both(k, 1 - y, 0).astype(bf16)
            go(ref, rs2.at[m(k)], rs2_r.at[m(k)], side)

        def line_slot(k, upward):
            return (flip if upward else 1 - flip) * depth + m(k)

        def sources(k):
            found = []
            if k >= u and down is not None:
                found.append(line_slot(k, True))
            if k <= u and up is not None:
                found.append(line_slot(k, False))
            return found

        def line_x(k):
            for b, yy in enumerate((1 - y, y)):
                total = both(k, yy, 1)
                for slot in sources(k):
                    got(rs3x.at[b, slot], rs3x_r.at[b, slot])
                    total = total + rs3x[b, slot].astype(f32)
                ref = span(k, yy, c, 1)
                if k != u:
                    ref[...] = total.astype(bf16)
                    slot = line_slot(k, k > u)
                    go(ref, rs3x.at[b, slot], rs3x_r.at[b, slot], z_dev(up if k > u else down))
                elif b == 0:
                    ref[...] = total.astype(bf16)
                    go(ref, rs4, rs4_r.at[0], side)
                else:
                    out_a[pl.ds(cut_r, rows - cut_r), :] = total

        def line_sum(k):
            got(rs2.at[m(k)], rs2_r.at[m(k)])
            total = both(k, y, 0) + rs2[m(k)].astype(f32)
            for slot in sources(k):
                got(rs3.at[slot], rs3_r.at[slot])
                total = total + rs3[slot].astype(f32)
            if k == u:
                out_a[pl.ds(0, cut_r), :] = fac[...] * total
            else:
                ref = span(k, y, c, 0)
                ref[...] = total.astype(bf16)
                slot = line_slot(k, k > u)
                go(ref, rs3.at[slot], rs3_r.at[slot], z_dev(up if k > u else down))

        def a_end():
            got(rs4, rs4_r.at[0])
            rest = pl.ds(cut_r, rows - cut_r)
            out_a[rest, :] = fac[...] * (out_a[rest, :] + rs4[...].astype(f32))

        lane = pl.multiple_of(c * half, 16)
        other = pl.multiple_of((1 - c) * half, 16)
        away = pl.multiple_of((1 - y) * quarter, 16)
        stay = pl.multiple_of(y * quarter, 16)
        mine = pl.multiple_of(lane + stay, 16)
        b_order = others[::-1] + [u]

        def cols_of(k):
            return pl.ds(pl.multiple_of(m(k) * chunk, 128), chunk)

        def b_part():
            got(low_r, x_r.at[1])
            weighted = coef[...] * (xs[1] + low_r[...].astype(f32))
            high = weighted.astype(bf16)
            rest = (weighted - high.astype(f32)).astype(bf16)
            for k in b_order:
                cols = cols_of(k)
                total = sum(
                    lax.dot_general(w, grad[:, cols], (((0,), (0,)), ((), ())), preferred_element_type=f32)
                    for w in (rest, high)
                )
                gb[:, cols] = total
                gbs[:, cols] = total.astype(bf16)
                go(gbs.at[pl.ds(other, half), cols], gb1.at[:, cols], g1_r.at[m(k)], core)

        def b_core(k):
            cols = cols_of(k)
            got(gb1.at[:, cols], g1_r.at[m(k)])
            gb2s[:, cols] = (
                gb[pl.ds(pl.multiple_of(lane + away, 16), quarter), cols]
                + gb1[pl.ds(away, quarter), cols].astype(f32)
            ).astype(bf16)
            go(gb2s.at[:, cols], gb2.at[:, cols], g2_r.at[m(k)], side)

        def b_side(k):
            cols = cols_of(k)
            got(gb2.at[:, cols], g2_r.at[m(k)])
            total = (
                gb[pl.ds(mine, quarter), cols]
                + gb1[pl.ds(stay, quarter), cols].astype(f32)
                + gb2[:, cols].astype(f32)
            )
            if k == u:
                gb[pl.ds(mine, quarter), cols] = total
            else:
                gb3s[:, cols] = total.astype(bf16)
                go(gb3s.at[:, cols], gb3.at[z], g3_r.at[z], z_dev(k))

        def final(k, yy, cc):
            at_row = pl.multiple_of(cc * half + yy * quarter, 16)
            return fin.at[pl.ds(at_row, quarter), cols_of(k)], fin_r.at[m(k) * 2 + yy]

        def b_send(k, yy, *devices):
            ref, sem = final(k, yy, c)
            for device in devices:
                go(ref, ref, sem if device is not core else fin_r.at[2 * depth], device)

        def b_line():
            cols = cols_of(u)
            total = gb[pl.ds(mine, quarter), cols]
            for k in others:
                got(gb3.at[m(k)], g3_r.at[m(k)])
                total = total + gb3[m(k)].astype(f32)
            scaled = jnp.full((1, 128), adapter_scale_factor) * fac[...]
            fin[pl.ds(mine, quarter), cols] = (scaled[:, :1] * total).astype(bf16)
            b_send(u, y, *[z_dev(k) for k in others[::-1]], side, core)

        def b_pass(k, yy):
            got(*final(k, yy, c))
            if yy is y:
                b_send(k, yy, side)
            b_send(k, yy, core)

        def b_end():
            got(fin.at[pl.ds(other, half)], fin_r.at[2 * depth])
            out_b[...] = fin[...].astype(f32)

        there = 1 - y
        plan = [
            (0.0, a_start), (0.1, back_send), (0.2, token_terms_here), (0.3, loss_one), (0.4, load_x.wait),
            (2.9, a_side, 2), (4.55, back_end), (4.7, a_side, 0), (6.4, a_side, 1), (7.2, loss_two), (21.5, loss_three),
        ]
        order = [k for k in (range(last, -1, -1)) if k > u] + [k for k in range(u)] + [u]
        for i, k in enumerate(order):
            plan.append((4.6 + 1.1 * i, part_of, k))
            plan.append((8.0 + 1.15 * i, core_wait, k))
            first = 17.35 if u == 0 else 11.35
            plan.append((max(first, 8.0 + 1.15 * i) + 0.01 * (i + 1), core_sum, k))
        if u == 0:
            for i, k in enumerate(order[:-1]):
                plan.append((8.05 + 1.15 * i, line_x, k))
        else:
            for k in order:
                if k > u:
                    plan.append((15.1 + 4.8 * (last - k), line_x, k))
                    plan.append((28.5 + 2.5 * (last - k), line_sum, k))
                elif k < u:
                    plan.append((21.7, line_x, k))
                    plan.append((33.0, line_sum, k))
                else:
                    plan.append((26.6, line_x, k))
        when = {}
        for k in others:
            hops = abs(k - u)
            when[k] = 3.5 + 6.0 * (hops - 1)
            plan.append((when[k], a_line, k, y, 0))
            plan.append((when[k] + 1.7, a_line, k, y, 1))
            plan.append((when[k] + 2.9, a_line, k, y, 2))
            plan.append((when[k] + 4.2, a_line, k, there, 2))
        queue = 4.7
        for i in (0, 1):
            for k in others:
                if u == 0 or abs(k - u) == 1:
                    queue = max(queue, when[k] + 1.7 * i) + 1.75 if u else when[k] + 1.7 * i + 1.75
                    when[k, i] = queue + (1.8 if u else 3.3)
                    plan.append((when[k, i], a_over, k, i))
        for i in (0, 1):
            for k in others:
                if u > 0 and abs(k - u) > 1:
                    queue = max(queue, when[k] + 1.7 * i) + 1.75
                    when[k, i] = queue + (1.8 if u else 3.3)
                    plan.append((when[k, i], a_over, k, i))
        for i, k in enumerate([u] + others):
            done = 9.0 if i == 0 else when[k, 1] + 1.2 + 0.1 * i
            if i < depth - 1 or depth == 1:
                plan.append((done, low_of, k, i == 0))
            else:
                plan.append((done - 0.6, low_near, k))
                plan.append((done, low_far, k))
        plan.append((done + 0.1, low_send))
        begin = done + 4.5
        if u == 0:
            plan.append((begin + 1.6, line_x, u))
            for k, moment in zip(order[:-1], (done + 0.15, done + 0.3, begin + 1.55)):
                plan.append((moment, line_sum, k))
        plan.append((begin, b_part))
        for i, k in enumerate(b_order):
            plan.append((begin + 1.5 + 0.01 * i, b_core, k))
            plan.append((begin + 4.5 + 0.9 * i, b_side, k))
        begin = max(begin, 6.0 * last + 10.3)
        plan.append((begin + 9.5, b_line))
        plan.append((begin + 13.9, line_sum, u))
        plan.append((begin + 13.91, a_end))
        plan.append((begin + 15.5, b_pass, u, there))
        for i, k in enumerate(others):
            plan.append((begin + 12.0 + 0.9 * i, b_pass, k, y))
            plan.append((begin + 14.0 + 0.9 * i, b_pass, k, there))
        plan.append((begin + 18.0, loss_end))
        plan.append((begin + 19.0, b_end))
        for entry in sorted(plan, key=lambda e: e[0]):
            name = getattr(entry[1], "__name__", "w") + "_".join(str(v) for v in entry[2:] if isinstance(v, int))
            with jax.named_scope(name) if SCOPES else contextlib.nullcontext():
                entry[1](*entry[2:])
        with jax.named_scope("drain") if SCOPES else contextlib.nullcontext():
            drain()

    for u in range((depth + 1) // 2):
        @pl.when(jnp.minimum(z, last - z) == u)
        def _():
            run(u)


def finish_kernel(a_in, b_in, loss_in, a_out, b_out, loss_out, sems):
    copies = [
        pltpu.make_async_copy(s, d, sems.at[i])
        for i, (s, d) in enumerate(((a_in, a_out), (b_in, b_out)))
    ]
    for copy in copies:
        copy.start()
    loss_out[0, 0] = loss_in[0, 0]
    for copy in copies:
        copy.wait()


def fused_local(activations, output_gradient, adapter_a, adapter_b, log_ratio, lengths, rewards):
    n = lax.axis_size("dp")
    depth = n // 4
    tokens, ff = activations.shape
    rows, rank = adapter_a.shape[1:]
    width = output_gradient.shape[1]
    dma = pltpu.SemaphoreType.DMA
    vmem, anywhere = pl.BlockSpec(memory_space=pltpu.VMEM), pl.BlockSpec(memory_space=pl.ANY)
    scalars = pl.BlockSpec(memory_space=pltpu.SMEM)
    hbm = pl.BlockSpec(memory_space=pltpu.HBM)
    quarter, chunk = rank // 4, width // depth
    cut_g, cut_r = rows * 3 // 64 * 16, rows // 32 * 16
    grad_a, grad_b, loss = pl.pallas_call(
        functools.partial(fused_kernel, n, lengths.shape[0], lengths.shape[1], cut_g, cut_r),
        out_shape=(
            jax.ShapeDtypeStruct((rows, rank), f32),
            jax.ShapeDtypeStruct((rank, width), f32),
            jax.ShapeDtypeStruct((8, 128), f32),
        ),
        in_specs=[hbm] * 7,
        out_specs=(vmem, vmem, vmem),
        scratch_shapes=[
            pltpu.VMEM((tokens // 128, 128), f32),
            pltpu.SMEM(lengths.shape, jnp.int32),
            pltpu.SMEM(rewards.shape, jnp.int32),
            pltpu.VMEM((tokens, ff), bf16),
            pltpu.VMEM((tokens, width), bf16),
            pltpu.VMEM((rank, width), bf16),
            pltpu.VMEM((ff, rank), bf16),
            pltpu.VMEM((ff, rank), bf16),
            pltpu.VMEM((2 * depth, rows, rank), bf16),
            pltpu.VMEM((depth, cut_r, rank), bf16),
            pltpu.VMEM((2 * depth, cut_r, rank), bf16),
            pltpu.VMEM((2, 2 * depth, rows - cut_r, rank), bf16),
            pltpu.VMEM((rows - cut_r, rank), bf16),
            pltpu.VMEM((2, tokens, rank), f32),
            pltpu.VMEM((tokens, rank), f32),
            pltpu.VMEM((tokens, rank), bf16),
            pltpu.VMEM((tokens, rank), bf16),
            pltpu.VMEM((tokens, rank), f32),
            pltpu.VMEM((tokens, rank), bf16),
            pltpu.VMEM((rank, width), f32),
            pltpu.VMEM((rank, width), bf16),
            pltpu.VMEM((rank // 2, width), bf16),
            pltpu.VMEM((quarter, width), bf16),
            pltpu.VMEM((quarter, width), bf16),
            pltpu.VMEM((quarter, width), bf16),
            pltpu.VMEM((depth, quarter, chunk), bf16),
            pltpu.VMEM((rank, width), bf16),
            pltpu.VMEM((2, 8, 128), f32),
            pltpu.VMEM((8, 128), f32),
            pltpu.VMEM((8, 128), f32),
            pltpu.VMEM((depth, 8, 128), f32),
            pltpu.VMEM((1, 128), f32),
            dma((7,)), dma((4,)), dma((6 * depth,)), dma((2 * depth,)),
            dma((depth,)), dma((depth,)), dma((2 * depth,)), dma((2, 2 * depth)), dma((1,)),
            dma((2,)), dma((depth,)), dma((depth,)), dma((depth,)), dma((2 * depth + 1,)),
            dma((2,)), dma((depth,)),
        ],
        compiler_params=pltpu.CompilerParams(
            collective_id=0, has_side_effects=True, vmem_limit_bytes=48 * 1024 * 1024
        ),
        name="fused",
    )(
        *(
            pltpu.with_memory_space_constraint(v, pltpu.HBM)
            for v in (
                activations, output_gradient, adapter_a[0], adapter_b,
                log_ratio.reshape(-1, 128), lengths, rewards,
            )
        )
    )
    grad_a, grad_b, loss = pl.pallas_call(
        finish_kernel,
        out_shape=(
            jax.ShapeDtypeStruct((rows, rank), f32),
            jax.ShapeDtypeStruct((rank, width), f32),
            jax.ShapeDtypeStruct((1, 1), f32),
        ),
        in_specs=[vmem, vmem, vmem],
        out_specs=(hbm, hbm, scalars),
        scratch_shapes=[dma((2,))],
        compiler_params=pltpu.CompilerParams(vmem_limit_bytes=4 * 1024 * 1024),
        name="finish",
    )(grad_a, grad_b, loss)
    return grad_a[None], grad_b, loss.reshape(())


def fits(mesh):
    n, split = mesh.shape["dp"], mesh.shape["tensor"]
    return n % 4 == 0 and 4 <= n <= 16 and split == 2


def local(activations, output_gradient, adapter_a, adapter_b, log_ratio, lengths, rewards):
    n = lax.axis_size("dp")
    rows, rank = adapter_a.shape[1:]
    width, ff = output_gradient.shape[1], activations.shape[1]
    small = 2 * activations.size + 8 * ff * rank < 32 * 1024 * 1024
    aligned = (
        rows % 16 == 0
        and rank == 128
        and activations.shape[0] % 128 == 0
        and ff % 128 == 0
        and 4 * rows % 128 == 0
        and rows >= 64
        and width % (128 * (n // 4)) == 0
        and n % lengths.shape[0] == 0
    )
    run = fused_local if small and aligned else plain_local
    return run(activations, output_gradient, adapter_a, adapter_b, log_ratio, lengths, rewards)


def solution(mesh):
    in_specs = (
        P("dp", "tensor"),
        P("dp", "tensor"),
        P("tensor", "dp", None),
        P(None, "tensor"),
        P("dp"),
        P(),
        P(),
    )
    out_specs = (P("tensor", "dp", None), P(None, "tensor"), P())
    body = local if fits(mesh) else plain_local
    return jax.shard_map(body, mesh=mesh, in_specs=in_specs, out_specs=out_specs, check_vma=False)
```

```python
import contextlib
import functools
import math

import jax
import jax.numpy as jnp
from jax import lax
from jax.experimental import pallas as pl
from jax.experimental.pallas import tpu as pltpu
from jax.sharding import PartitionSpec as P

clip_eps = 0.2
adapter_scale_factor = 2.0


def token_terms(length_row, reward_row, log_ratio, offset):
    reward = reward_row.astype(jnp.float32)
    center = jnp.mean(reward)
    spread = jnp.mean((reward - center) * (reward - center))
    advantage = (reward - center) / jnp.sqrt(spread + 1.0)
    ends = jnp.cumsum(length_row)
    starts = ends - length_row
    slots = jnp.arange(log_ratio.shape[0], dtype=jnp.int32) + offset
    member = ((slots[None, :] >= starts[:, None]) & (slots[None, :] < ends[:, None])).astype(
        jnp.float32
    )
    live = jnp.sum(member, axis=0)
    token_adv = jnp.sum(member * advantage[:, None], axis=0)
    ratio = jnp.exp(log_ratio)
    unclipped = ratio * token_adv
    clipped = jnp.clip(ratio, 1.0 - clip_eps, 1.0 + clip_eps) * token_adv
    token_loss = -jnp.minimum(unclipped, clipped)
    slope = jnp.where(unclipped <= clipped, -unclipped, jnp.zeros_like(unclipped))
    return (live * slope, jnp.sum(live * token_loss), jnp.sum(live))


def plain_local(activations, output_gradient, adapter_a, adapter_b, log_ratio, lengths, rewards):
    tokens = activations.shape[0]
    groups = lengths.shape[0]
    per_group = lax.axis_size("dp") // groups
    position = lax.axis_index("dp")
    group_id = position // per_group
    offset = position % per_group * tokens
    length_row = lax.dynamic_index_in_dim(lengths, group_id, 0, keepdims=False)
    reward_row = lax.dynamic_index_in_dim(rewards, group_id, 0, keepdims=False)
    token_coefficient, loss_local, live_count = token_terms(
        length_row, reward_row, log_ratio, offset
    )
    columns = activations
    partial_low = jnp.dot(
        columns,
        lax.all_gather(adapter_a, "dp", axis=1, tiled=True)[0],
        preferred_element_type=jnp.float32,
    )
    partial_back = lax.dot_general(
        output_gradient, adapter_b, (((1,), (1,)), ((), ())), preferred_element_type=jnp.float32
    )
    low_rank, backward_projection = lax.psum((partial_low, partial_back), "tensor")
    error_rows = (adapter_scale_factor * token_coefficient[:, None] * backward_projection).astype(
        jnp.bfloat16
    )
    weighted_error = token_coefficient[:, None] * low_rank
    local_adapter_b_gradient = adapter_scale_factor * jnp.einsum(
        "tr,td->rd",
        weighted_error,
        output_gradient.astype(jnp.float32),
        precision=lax.Precision.HIGHEST,
    )
    columns = activations
    grad_a = lax.psum_scatter(
        lax.dot_general(
            columns, error_rows, (((0,), (0,)), ((), ())), preferred_element_type=jnp.float32
        ),
        "dp",
        scatter_dimension=0,
        tiled=True,
    )
    grad_b_sum, loss_sum, live_sum = lax.psum(
        (local_adapter_b_gradient, loss_local, live_count), "dp"
    )
    factor = groups / live_sum
    return ((factor * grad_a)[None], factor * grad_b_sum, factor * loss_sum)


MESH = pl.DeviceIdType.MESH
f32, bf16 = jnp.float32, jnp.bfloat16


def tile_of(total, most):
    return max(k for k in range(128, most + 1, 128) if total % k == 0)


SCOPES = False


def fused_kernel(
    n, groups, rollouts, cut_g, cut_r,
    act_hbm, grad_hbm, a_hbm, b_hbm, ratio_hbm, len_hbm, rew_hbm,
    out_a, out_b, out_loss,
    ratio_ref, len_ref, rew_ref,
    act, grad, b_mat, a_all, part, rs1, rs2, rs3, rs3x, rs4, xs, back_s, back_r, low_s, low_r, coef, err,
    gb, gbs, gb1, gb2s, gb2, gb3s, gb3, fin, ls, l1, l2, lz,
    fac, loc, send_s, ag_r, ag_c, rs1_r, rs2_r, rs3_r, rs3x_r, rs4_r,
    x_r, g1_r, g2_r, g3_r, fin_r, l_r, lz_r,
):
    depth = n // 4
    last = depth - 1
    p = lax.axis_index("dp")
    t = lax.axis_index("tensor")
    c, y, z = p % 2, (p // 2) % 2, p // 4
    tokens, ff = act.shape
    rows, rank = a_hbm.shape
    width = grad.shape[1]
    chunk = width // depth

    def at(zz, yy, cc):
        return (zz * 2 + yy) * 2 + cc

    def remote(s, d, ss, rs, dev, tensor=None):
        return pltpu.make_async_remote_copy(
            src_ref=s, dst_ref=d, send_sem=ss, recv_sem=rs,
            device_id=(dev, t if tensor is None else tensor), device_id_type=MESH,
        )

    core, side = at(z, y, 1 - c), at(z, 1 - y, c)

    load_a = pltpu.make_async_copy(a_hbm, a_all.at[pl.ds(pl.multiple_of(p * rows, 16), rows)], loc.at[0])
    load_g = pltpu.make_async_copy(grad_hbm, grad, loc.at[1])
    load_b = pltpu.make_async_copy(b_hbm, b_mat, loc.at[2])
    load_x = pltpu.make_async_copy(act_hbm, act, loc.at[3])
    small = [
        pltpu.make_async_copy(s, d, loc.at[4 + i])
        for i, (s, d) in enumerate(((ratio_hbm, ratio_ref), (len_hbm, len_ref), (rew_hbm, rew_ref)))
    ]
    barrier = pltpu.get_barrier_semaphore()
    for dev in [core, side] + [at((z + k) % depth, y, c) for k in range(1, depth)]:
        pl.semaphore_signal(barrier, inc=1, device_id=(dev, t), device_id_type=MESH)
    pl.semaphore_signal(barrier, inc=1, device_id=(p, 1 - t), device_id_type=MESH)
    for copy in [load_a, load_g, load_b] + small + [load_x]:
        copy.start()
    load_a.wait()
    with jax.named_scope("barrier") if SCOPES else contextlib.nullcontext():
        pl.semaphore_wait(barrier, depth + 2)
    flip = (2 * z > last).astype(jnp.int32)
    tile = tile_of(4 * rows, 1280)
    steps = 4 * rows // tile

    def run(u, own):
        sent = []
        mate = 1 - own

        def m(k):
            return k + flip * (last - 2 * k)

        def dev(k, yy, cc):
            return at(m(k), yy, cc)

        there = 1 - y
        others = sorted((k for k in range(depth) if k != u), key=lambda k: abs(k - u))
        up = u + 1 if u < last else None
        down = u - 1 if u > 0 else None

        def onward(k):
            return up if k < u else down

        def go(s, d, rs, device, tensor=None):
            size = s.dtype.itemsize * math.prod(s.shape) // 256
            if not sent or sent[-1] + size > ff:
                sent.append(0)
            sent[-1] += size
            remote(s, d, send_s.at[len(sent) - 1], rs, device, tensor).start()

        def drain():
            for i, size in enumerate(sent):
                ref = a_all.at[pl.ds(0, size)]
                remote(ref, ref, send_s.at[i], send_s.at[i], core).wait_send()

        def got(d, rs):
            remote(d, d, send_s.at[0], rs, core).wait_recv()

        def z_dev(k):
            return dev(k, y, c)

        middle = cut_g // 32 * 16
        first_rows = [(0, middle), (middle, cut_g)]
        carried = [(own, low, high, True) for low, high in first_rows]
        if own == 1:
            carried += [(cc, cut_g, rows, False) for cc in (1, 0)]

        def rows_of(k, yy, cc, low, high):
            return a_all.at[pl.ds(pl.multiple_of(dev(k, yy, cc) * rows + low, 16), high - low)]

        def piece(k, yy, i):
            return rows_of(k, yy, *carried[i][:3]), ag_r.at[(m(k) * 2 + yy) * 4 + i]

        def a_send(k, yy, i, *devices):
            ref, sem = piece(k, yy, i)
            for device in devices:
                if device is not None:
                    go(ref, ref, sem if device is not core else ag_c.at[m(k) * 2 + yy], device)

        def a_wait(k, yy, i):
            got(*piece(k, yy, i))

        def a_core(k, yy):
            size = cut_g
            if own == 0:
                size = rows if k == u and yy is y else 2 * rows - cut_g
            got(a_all.at[pl.ds(0, size)], ag_c.at[m(k) * 2 + yy])

        up_dev = None if up is None else z_dev(up)
        down_dev = None if down is None else z_dev(down)
        line = (up_dev, down_dev)

        def a_start():
            a_send(u, y, 0, *line)
            if own == 0:
                ref = rows_of(u, y, 0, cut_g, rows)
                go(ref, ref, ag_c.at[2 * depth], core)
                a_send(u, y, 1, *line)
                a_send(u, y, 0, side)
                a_send(u, y, 1, side)
            else:
                a_send(u, y, 2, side)
                a_send(u, y, 1, *line)
                a_send(u, y, 2, *line)
            for i in range(2 + own):
                a_send(u, y, i, core)

        def a_mate():
            got(rows_of(u, y, 0, cut_g, rows), ag_c.at[2 * depth])
            a_send(u, y, 3, side, *line)
            a_send(u, y, 0, side)
            a_send(u, y, 1, side)

        def a_side(i):
            a_wait(u, 1 - y, i)
            if not carried[i][3]:
                a_send(u, 1 - y, i, *line)
            a_send(u, 1 - y, i, core)

        def a_line(k, yy, i):
            a_wait(k, yy, i)
            to = onward(k)
            a_send(k, yy, i, None if to is None else z_dev(to))
            if carried[i][3]:
                a_send(k, yy, i, side)
            a_send(k, yy, i, core)

        def a_over(k, i):
            a_wait(k, 1 - y, i)
            a_send(k, 1 - y, i, core)

        def low_rows(start, size, first=False):
            width_of = size if size <= 2048 else tile_of(size, 1280)

            def step(i, total):
                cols = pl.ds(pl.multiple_of(start + i * width_of, 128), width_of)
                return total + jnp.dot(act[:, cols], a_all[cols, :], preferred_element_type=f32)

            begin = jnp.zeros((tokens, rank), f32) if first else xs[1]
            xs[1] = lax.fori_loop(0, size // width_of, step, begin)

        def low_of(k, first):
            for yy in (y, there):
                a_core(k, yy)
            low_rows(m(k) * (4 * rows), 4 * rows, first)

        small_part = 2 * rows // 128 * 128

        def low_near(k):
            a_core(k, y)
            low_rows(m(k) * (4 * rows) + y * (4 * rows - small_part), small_part)

        def low_far(k):
            a_core(k, 1 - y)
            low_rows(m(k) * (4 * rows) + (1 - y) * small_part, 4 * rows - small_part)

        def low_send():
            low_s[...] = xs[1].astype(bf16)
            go(low_s, low_r, x_r.at[1], p, 1 - t)

        def loss_one():
            go(ls.at[0], l1, l_r.at[0], core)

        def loss_two():
            got(l1, l_r.at[0])
            ls[1] = ls[0] + l1[...]
            go(ls.at[1], l2, l_r.at[1], side)

        def loss_three():
            got(l2, l_r.at[1])
            lz[z] = ls[1] + l2[...]
            for k in others:
                go(lz.at[z], lz.at[z], lz_r.at[z], z_dev(k))

        def loss_end():
            for k in others:
                got(lz.at[m(k)], lz_r.at[m(k)])
            total = lz[0]
            for i in range(1, depth):
                total = total + lz[i]
            out_loss[...] = fac[...] * total

        def back_send():
            load_g.wait()
            load_b.wait()
            xs[0] = lax.dot_general(
                grad[...], b_mat[...], (((1,), (1,)), ((), ())), preferred_element_type=f32
            )
            back_s[...] = xs[0].astype(bf16)
            go(back_s, back_r, x_r.at[0], p, 1 - t)

        def token_terms_here():
            for copy in small:
                copy.wait()
            per_group = n // groups
            group = p // per_group
            offset = (p % per_group) * tokens
            slots = (
                lax.broadcasted_iota(jnp.int32, ratio_ref.shape, 0) * 128
                + lax.broadcasted_iota(jnp.int32, ratio_ref.shape, 1)
                + offset
            )
            live_total = jnp.int32(0)
            live = jnp.zeros(ratio_ref.shape, f32)
            token_adv = jnp.zeros(ratio_ref.shape, f32)
            for g in range(groups):
                here = jnp.full((1, 128), (group == g).astype(f32))
                reward = [jnp.full((1, 128), rew_ref[g, i]).astype(f32) for i in range(rollouts)]
                center = sum(reward) / rollouts
                spread = sum((r - center) * (r - center) for r in reward) / rollouts
                scale = jnp.sqrt(spread + 1.0)
                end = jnp.int32(0)
                for i in range(rollouts):
                    start = end
                    end = end + len_ref[g, i]
                    member = ((slots >= start) & (slots < end)).astype(f32) * here
                    live = live + member
                    token_adv = token_adv + member * ((reward[i] - center) / scale)
                live_total = live_total + jnp.minimum(end, per_group * tokens)
            ratio = jnp.exp(ratio_ref[...])
            unclipped = ratio * token_adv
            clipped = jnp.clip(ratio, 1.0 - clip_eps, 1.0 + clip_eps) * token_adv
            token_loss = -jnp.minimum(unclipped, clipped)
            slope = jnp.where(unclipped <= clipped, -unclipped, jnp.zeros_like(unclipped))
            weight = live * slope
            for i in range(tokens // 128):
                coef[pl.ds(i * 128, 128), :] = jnp.broadcast_to(weight[i : i + 1, :], (128, 128)).T
            fac[...] = groups / jnp.full((1, 128), live_total).astype(f32)
            loss_part = jnp.sum(jnp.sum(live * token_loss, axis=1, keepdims=True), axis=0, keepdims=True)
            ls[0] = jnp.broadcast_to(loss_part, (8, 128))

        def back_end():
            got(back_r, x_r.at[0])
            err[...] = (adapter_scale_factor * coef[...] * (xs[0] + back_r[...].astype(f32))).astype(bf16)

        def span(k, yy, cc, part_two=None):
            q = dev(k, yy, cc)
            low, size = {None: (0, rows), 0: (0, cut_r), 1: (cut_r, rows - cut_r)}[part_two]
            return part.at[pl.ds(pl.multiple_of(q * rows + low, 16), size)]

        def part_of(k):
            base = m(k) * (4 * rows)

            def step(i, _):
                cols = pl.ds(pl.multiple_of(base + i * tile, 128), tile)
                part[cols, :] = lax.dot_general(
                    act[:, cols], err[...], (((0,), (0,)), ((), ())), preferred_element_type=f32
                ).astype(bf16)
                return 0

            lax.fori_loop(0, steps, step, 0)
            for yy in (1 - y, y):
                slot = m(k) * 2 + yy
                go(span(k, yy, 1 - c), rs1.at[slot], rs1_r.at[m(k)], core)

        def both(k, yy, i):
            low, size = (0, cut_r) if i == 0 else (cut_r, rows - cut_r)
            return span(k, yy, c, i)[...].astype(f32) + rs1[m(k) * 2 + yy, pl.ds(low, size), :].astype(f32)

        def core_wait(k):
            got(rs1.at[pl.ds(m(k) * 2, 2)], rs1_r.at[m(k)])

        def core_sum(k):
            ref = span(k, 1 - y, c, 0)
            ref[...] = both(k, 1 - y, 0).astype(bf16)
            go(ref, rs2.at[m(k)], rs2_r.at[m(k)], side)

        def line_slot(k, upward):
            return (flip if upward else 1 - flip) * depth + m(k)

        def sources(k):
            found = []
            if k >= u and down is not None:
                found.append(line_slot(k, True))
            if k <= u and up is not None:
                found.append(line_slot(k, False))
            return found

        def line_x(k):
            for slot in sources(k):
                got(rs3x.at[slot], rs3x_r.at[slot])
            for b, yy in enumerate((1 - y, y)):
                total = both(k, yy, 1)
                for slot in sources(k):
                    total = total + rs3x[slot, b].astype(f32)
                ref = span(k, yy, c, 1)
                if k != u:
                    ref[...] = total.astype(bf16)
                    slot = line_slot(k, k > u)
                    go(ref, rs3x.at[slot, b], rs3x_r.at[slot], z_dev(up if k > u else down))
                elif b == 0:
                    ref[...] = total.astype(bf16)
                    go(ref, rs4, rs4_r.at[0], side)
                else:
                    out_a[pl.ds(cut_r, rows - cut_r), :] = total

        def line_sum(k):
            got(rs2.at[m(k)], rs2_r.at[m(k)])
            total = both(k, y, 0) + rs2[m(k)].astype(f32)
            for slot in sources(k):
                got(rs3.at[slot], rs3_r.at[slot])
                total = total + rs3[slot].astype(f32)
            if k == u:
                out_a[pl.ds(0, cut_r), :] = fac[...] * total
            else:
                ref = span(k, y, c, 0)
                ref[...] = total.astype(bf16)
                slot = line_slot(k, k > u)
                go(ref, rs3.at[slot], rs3_r.at[slot], z_dev(up if k > u else down))

        def a_end():
            got(rs4, rs4_r.at[0])
            rest = pl.ds(cut_r, rows - cut_r)
            out_a[rest, :] = fac[...] * (out_a[rest, :] + rs4[...].astype(f32))

        bases, halves, quarters = (0, rank // 4), (rank // 4, rank * 3 // 4), (rank // 8, rank * 3 // 8)
        lane, other, quarter = bases[own], bases[mate], quarters[own]
        whole = pl.ds(0, quarter)
        away = pl.multiple_of((1 - y) * quarter, 16)
        stay = pl.multiple_of(y * quarter, 16)
        mine = pl.multiple_of(lane + stay, 16)
        b_order = others[::-1] + [u]

        def cols_of(k):
            return pl.ds(pl.multiple_of(m(k) * chunk, 128), chunk)

        def b_part():
            got(low_r, x_r.at[1])
            weighted = coef[...] * (xs[1] + low_r[...].astype(f32))
            high = weighted.astype(bf16)
            rest = (weighted - high.astype(f32)).astype(bf16)
            for k in b_order:
                cols = cols_of(k)
                total = sum(
                    lax.dot_general(w, grad[:, cols], (((0,), (0,)), ((), ())), preferred_element_type=f32)
                    for w in (rest, high)
                )
                gb[:, cols] = total
                gbs[:, cols] = total.astype(bf16)
                rest_rows = pl.ds(0, halves[mate])
                go(gbs.at[pl.ds(other, halves[mate]), cols], gb1.at[rest_rows, cols], g1_r.at[m(k)], core)

        def b_core(k):
            cols = cols_of(k)
            got(gb1.at[pl.ds(0, halves[own]), cols], g1_r.at[m(k)])
            gb2s[whole, cols] = (
                gb[pl.ds(pl.multiple_of(lane + away, 16), quarter), cols]
                + gb1[pl.ds(away, quarter), cols].astype(f32)
            ).astype(bf16)
            go(gb2s.at[whole, cols], gb2.at[whole, cols], g2_r.at[m(k)], side)

        def b_side(k):
            cols = cols_of(k)
            got(gb2.at[whole, cols], g2_r.at[m(k)])
            total = (
                gb[pl.ds(mine, quarter), cols]
                + gb1[pl.ds(stay, quarter), cols].astype(f32)
                + gb2[whole, cols].astype(f32)
            )
            if k == u:
                gb[pl.ds(mine, quarter), cols] = total
            else:
                gb3s[whole, cols] = total.astype(bf16)
                go(gb3s.at[whole, cols], gb3.at[z, whole], g3_r.at[z], z_dev(k))

        def final(k, yy, cc):
            at_row = pl.multiple_of(bases[cc] + yy * quarters[cc], 16)
            return fin.at[pl.ds(at_row, quarters[cc]), cols_of(k)], fin_r.at[m(k) * 2 + yy]

        def b_send(k, yy, *devices):
            ref, sem = final(k, yy, own)
            for device in devices:
                go(ref, ref, sem if device is not core else fin_r.at[2 * depth], device)

        def b_line():
            cols = cols_of(u)
            total = gb[pl.ds(mine, quarter), cols]
            for k in others:
                got(gb3.at[m(k), whole], g3_r.at[m(k)])
                total = total + gb3[m(k), whole, :].astype(f32)
            scaled = jnp.full((1, 128), adapter_scale_factor) * fac[...]
            fin[pl.ds(mine, quarter), cols] = (scaled[:, :1] * total).astype(bf16)
            b_send(u, y, *[z_dev(k) for k in others[::-1]], side, core)

        def b_pass(k, yy):
            got(*final(k, yy, own))
            if yy is y and abs(k - u) > 1:
                b_send(k, yy, side)
            if k == u:
                b_send(k, yy, *[device for device in (up_dev, down_dev) if device is not None])
            b_send(k, yy, core)

        def b_end():
            got(fin.at[pl.ds(other, halves[mate])], fin_r.at[2 * depth])
            out_b[...] = fin[...].astype(f32)

        plan = [
            (0.0, a_start), (0.1, back_send), (0.2, token_terms_here), (0.3, loss_one), (0.4, load_x.wait),
            (4.55, back_end), (7.2, loss_two), (21.5, loss_three),
        ]
        order = [k for k in (range(last, -1, -1)) if k > u] + [k for k in range(u)] + [u]
        for i, k in enumerate(order):
            plan.append((4.6 + 1.1 * i, part_of, k))
            ready = 7.3 + 1.15 * i
            plan.append((ready, core_wait, k))
            first = ready if i == 0 else (17.35 if u == 0 else 11.35)
            plan.append((max(first, ready) + 0.01 * (i + 1), core_sum, k))
        if u == 0:
            for i, k in enumerate(order[:-1]):
                plan.append((7.35 + 1.15 * i if i < 2 else 15.4, line_x, k))
            plan.append((15.3, line_sum, order[0]))
        else:
            for k in order:
                if k > u:
                    plan.append((15.1 + 4.8 * (last - k), line_x, k))
                    plan.append((21.8 + 8.6 * (last - k), line_sum, k))
                elif k < u:
                    plan.append((21.7, line_x, k))
                    plan.append((30.3, line_sum, k))
                else:
                    plan.append((26.6, line_x, k))
        if own == 0:
            plan += [(4.4, a_side, 0), (6.2, a_side, 1)]
        else:
            plan += [(0.35, a_mate), (2.9, a_side, 2), (4.2, a_side, 3), (6.0, a_side, 0), (7.7, a_side, 1)]
        when = {}
        for core_id in (0, 1):
            moments = {}
            for k in others:
                hops = abs(k - u)
                moments[k] = 4.35 * hops if core_id == 0 else 3.5 + 6.0 * (hops - 1)
            queue, crossing = 4.7, 2.7 if core_id == 0 else 1.8
            arrivals = sorted((moments[k] + 1.7 * i, k, i) for k in others for i in (0, 1))
            for moment, k, i in arrivals:
                queue = max(queue, moment) + 1.75
                when[k, i] = max(when.get((k, i), 0), queue + crossing)
                if core_id == own:
                    plan.append((moment, a_line, k, y, i))
                    plan.append((queue + crossing + 1.0, a_over, k, i))
            if core_id == own == 1:
                for k in others:
                    for i in (2, 3):
                        plan.append((moments[k] + 1.6 + 0.6 * i, a_line, k, y, i))
                        plan.append((moments[k] + 2.8 + 0.6 * i, a_line, k, there, i))
        for i, k in enumerate([u] + others):
            done = 9.0 if i == 0 else when[k, 1] + 1.2 + 0.1 * i
            if i < depth - 1 or depth == 1:
                plan.append((done, low_of, k, i == 0))
            else:
                plan.append((done - 0.6, low_near, k))
                plan.append((done, low_far, k))
        plan.append((done + 0.1, low_send))
        begin = done + 4.5
        if u == 0:
            plan.append((begin + 1.6, line_x, u))
            for k, moment in zip(order[1:-1], (done + 0.15, done + 0.3)):
                plan.append((moment, line_sum, k))
        plan.append((begin, b_part))
        for i, k in enumerate(b_order):
            plan.append((begin + 1.5 + 0.01 * i, b_core, k))
            plan.append((begin + 4.5 + 0.9 * i, b_side, k))
        begin = max(begin, 6.0 * last + 10.3)
        plan.append((begin + 9.5, b_line))
        plan.append((begin + 12.9, line_sum, u))
        plan.append((begin + 12.91, a_end))
        plan.append((begin + 12.0, b_pass, u, there))
        for i, k in enumerate(others):
            plan.append((begin + 12.1 + 0.01 * (last - i), b_pass, k, y))
            plan.append((begin + 14.0 + 0.9 * i, b_pass, k, there))
        plan.append((begin + 18.0, loss_end))
        plan.append((begin + 19.0, b_end))
        for entry in sorted(plan, key=lambda e: e[0]):
            name = getattr(entry[1], "__name__", "w") + "_".join(str(v) for v in entry[2:] if isinstance(v, int))
            with jax.named_scope(name) if SCOPES else contextlib.nullcontext():
                entry[1](*entry[2:])
        with jax.named_scope("drain") if SCOPES else contextlib.nullcontext():
            drain()

    for u in range((depth + 1) // 2):
        for own in (0, 1):
            @pl.when((jnp.minimum(z, last - z) == u) & (c == own))
            def _():
                run(u, own)


def finish_kernel(a_in, b_in, loss_in, a_out, b_out, loss_out, sems):
    copies = [
        pltpu.make_async_copy(s, d, sems.at[i])
        for i, (s, d) in enumerate(((a_in, a_out), (b_in, b_out)))
    ]
    for copy in copies:
        copy.start()
    loss_out[0, 0] = loss_in[0, 0]
    for copy in copies:
        copy.wait()


def fused_local(activations, output_gradient, adapter_a, adapter_b, log_ratio, lengths, rewards):
    n = lax.axis_size("dp")
    depth = n // 4
    tokens, ff = activations.shape
    rows, rank = adapter_a.shape[1:]
    width = output_gradient.shape[1]
    dma = pltpu.SemaphoreType.DMA
    vmem, anywhere = pl.BlockSpec(memory_space=pltpu.VMEM), pl.BlockSpec(memory_space=pl.ANY)
    scalars = pl.BlockSpec(memory_space=pltpu.SMEM)
    hbm = pl.BlockSpec(memory_space=pltpu.HBM)
    quarter, chunk = rank // 4, width // depth
    quarter = rank * 3 // 8
    cut_g, cut_r = rows * 3 // 64 * 16, rows // 32 * 16
    grad_a, grad_b, loss = pl.pallas_call(
        functools.partial(fused_kernel, n, lengths.shape[0], lengths.shape[1], cut_g, cut_r),
        out_shape=(
            jax.ShapeDtypeStruct((rows, rank), f32),
            jax.ShapeDtypeStruct((rank, width), f32),
            jax.ShapeDtypeStruct((8, 128), f32),
        ),
        in_specs=[hbm] * 7,
        out_specs=(vmem, vmem, vmem),
        scratch_shapes=[
            pltpu.VMEM((tokens // 128, 128), f32),
            pltpu.SMEM(lengths.shape, jnp.int32),
            pltpu.SMEM(rewards.shape, jnp.int32),
            pltpu.VMEM((tokens, ff), bf16),
            pltpu.VMEM((tokens, width), bf16),
            pltpu.VMEM((rank, width), bf16),
            pltpu.VMEM((ff, rank), bf16),
            pltpu.VMEM((ff, rank), bf16),
            pltpu.VMEM((2 * depth, rows, rank), bf16),
            pltpu.VMEM((depth, cut_r, rank), bf16),
            pltpu.VMEM((2 * depth, cut_r, rank), bf16),
            pltpu.VMEM((2 * depth, 2, rows - cut_r, rank), bf16),
            pltpu.VMEM((rows - cut_r, rank), bf16),
            pltpu.VMEM((2, tokens, rank), f32),
            pltpu.VMEM((tokens, rank), bf16),
            pltpu.VMEM((tokens, rank), bf16),
            pltpu.VMEM((tokens, rank), bf16),
            pltpu.VMEM((tokens, rank), bf16),
            pltpu.VMEM((tokens, rank), f32),
            pltpu.VMEM((tokens, rank), bf16),
            pltpu.VMEM((rank, width), f32),
            pltpu.VMEM((rank, width), bf16),
            pltpu.VMEM((rank * 3 // 4, width), bf16),
            pltpu.VMEM((quarter, width), bf16),
            pltpu.VMEM((quarter, width), bf16),
            pltpu.VMEM((quarter, width), bf16),
            pltpu.VMEM((depth, quarter, chunk), bf16),
            pltpu.VMEM((rank, width), bf16),
            pltpu.VMEM((2, 8, 128), f32),
            pltpu.VMEM((8, 128), f32),
            pltpu.VMEM((8, 128), f32),
            pltpu.VMEM((depth, 8, 128), f32),
            pltpu.VMEM((1, 128), f32),
            dma((7,)), dma((4,)), dma((8 * depth,)), dma((2 * depth + 1,)),
            dma((depth,)), dma((depth,)), dma((2 * depth,)), dma((2 * depth,)), dma((1,)),
            dma((2,)), dma((depth,)), dma((depth,)), dma((depth,)), dma((2 * depth + 1,)),
            dma((2,)), dma((depth,)),
        ],
        compiler_params=pltpu.CompilerParams(
            collective_id=0, has_side_effects=True, vmem_limit_bytes=48 * 1024 * 1024
        ),
        name="fused",
    )(
        *(
            pltpu.with_memory_space_constraint(v, pltpu.HBM)
            for v in (
                activations, output_gradient, adapter_a[0], adapter_b,
                log_ratio.reshape(-1, 128), lengths, rewards,
            )
        )
    )
    grad_a, grad_b, loss = pl.pallas_call(
        finish_kernel,
        out_shape=(
            jax.ShapeDtypeStruct((rows, rank), f32),
            jax.ShapeDtypeStruct((rank, width), f32),
            jax.ShapeDtypeStruct((1, 1), f32),
        ),
        in_specs=[vmem, vmem, vmem],
        out_specs=(hbm, hbm, scalars),
        scratch_shapes=[dma((2,))],
        compiler_params=pltpu.CompilerParams(vmem_limit_bytes=4 * 1024 * 1024),
        name="finish",
    )(grad_a, grad_b, loss)
    return grad_a[None], grad_b, loss.reshape(())


def fits(mesh):
    n, split = mesh.shape["dp"], mesh.shape["tensor"]
    return n % 4 == 0 and 4 <= n <= 16 and split == 2


def local(activations, output_gradient, adapter_a, adapter_b, log_ratio, lengths, rewards):
    n = lax.axis_size("dp")
    rows, rank = adapter_a.shape[1:]
    width, ff = output_gradient.shape[1], activations.shape[1]
    small = 2 * activations.size + 8 * ff * rank < 32 * 1024 * 1024
    aligned = (
        rows % 16 == 0
        and rank == 128
        and activations.shape[0] % 128 == 0
        and ff % 128 == 0
        and 4 * rows % 128 == 0
        and rows % 32 == 0
        and rows >= 64
        and width % (128 * (n // 4)) == 0
        and n % lengths.shape[0] == 0
    )
    run = fused_local if small and aligned else plain_local
    return run(activations, output_gradient, adapter_a, adapter_b, log_ratio, lengths, rewards)


def solution(mesh):
    in_specs = (
        P("dp", "tensor"),
        P("dp", "tensor"),
        P("tensor", "dp", None),
        P(None, "tensor"),
        P("dp"),
        P(),
        P(),
    )
    out_specs = (P("tensor", "dp", None), P(None, "tensor"), P())
    body = local if fits(mesh) else plain_local
    return jax.shard_map(body, mesh=mesh, in_specs=in_specs, out_specs=out_specs, check_vma=False)
```

```python
import contextlib
import functools
import math

import jax
import jax.numpy as jnp
from jax import lax
from jax.experimental import pallas as pl
from jax.experimental.pallas import tpu as pltpu
from jax.sharding import PartitionSpec as P

clip_eps = 0.2
adapter_scale_factor = 2.0


def token_terms(length_row, reward_row, log_ratio, offset):
    reward = reward_row.astype(jnp.float32)
    center = jnp.mean(reward)
    spread = jnp.mean((reward - center) * (reward - center))
    advantage = (reward - center) / jnp.sqrt(spread + 1.0)
    ends = jnp.cumsum(length_row)
    starts = ends - length_row
    slots = jnp.arange(log_ratio.shape[0], dtype=jnp.int32) + offset
    member = ((slots[None, :] >= starts[:, None]) & (slots[None, :] < ends[:, None])).astype(
        jnp.float32
    )
    live = jnp.sum(member, axis=0)
    token_adv = jnp.sum(member * advantage[:, None], axis=0)
    ratio = jnp.exp(log_ratio)
    unclipped = ratio * token_adv
    clipped = jnp.clip(ratio, 1.0 - clip_eps, 1.0 + clip_eps) * token_adv
    token_loss = -jnp.minimum(unclipped, clipped)
    slope = jnp.where(unclipped <= clipped, -unclipped, jnp.zeros_like(unclipped))
    return (live * slope, jnp.sum(live * token_loss), jnp.sum(live))


def plain_local(activations, output_gradient, adapter_a, adapter_b, log_ratio, lengths, rewards):
    tokens = activations.shape[0]
    groups = lengths.shape[0]
    per_group = lax.axis_size("dp") // groups
    position = lax.axis_index("dp")
    group_id = position // per_group
    offset = position % per_group * tokens
    length_row = lax.dynamic_index_in_dim(lengths, group_id, 0, keepdims=False)
    reward_row = lax.dynamic_index_in_dim(rewards, group_id, 0, keepdims=False)
    token_coefficient, loss_local, live_count = token_terms(
        length_row, reward_row, log_ratio, offset
    )
    columns = activations
    partial_low = jnp.dot(
        columns,
        lax.all_gather(adapter_a, "dp", axis=1, tiled=True)[0],
        preferred_element_type=jnp.float32,
    )
    partial_back = lax.dot_general(
        output_gradient, adapter_b, (((1,), (1,)), ((), ())), preferred_element_type=jnp.float32
    )
    low_rank, backward_projection = lax.psum((partial_low, partial_back), "tensor")
    error_rows = (adapter_scale_factor * token_coefficient[:, None] * backward_projection).astype(
        jnp.bfloat16
    )
    weighted_error = token_coefficient[:, None] * low_rank
    local_adapter_b_gradient = adapter_scale_factor * jnp.einsum(
        "tr,td->rd",
        weighted_error,
        output_gradient.astype(jnp.float32),
        precision=lax.Precision.HIGHEST,
    )
    columns = activations
    grad_a = lax.psum_scatter(
        lax.dot_general(
            columns, error_rows, (((0,), (0,)), ((), ())), preferred_element_type=jnp.float32
        ),
        "dp",
        scatter_dimension=0,
        tiled=True,
    )
    grad_b_sum, loss_sum, live_sum = lax.psum(
        (local_adapter_b_gradient, loss_local, live_count), "dp"
    )
    factor = groups / live_sum
    return ((factor * grad_a)[None], factor * grad_b_sum, factor * loss_sum)


MESH = pl.DeviceIdType.MESH
f32, bf16 = jnp.float32, jnp.bfloat16


def tile_of(total, most):
    return max(k for k in range(128, most + 1, 128) if total % k == 0)


SCOPES = False


def fused_kernel(
    n, groups, rollouts, cut_g, cut_r,
    act_hbm, grad_hbm, a_hbm, b_hbm, ratio_hbm, len_hbm, rew_hbm,
    out_a, out_b, out_loss,
    ratio_ref, len_ref, rew_ref,
    act, grad, b_mat, a_all, part, rs1, rs2, rs3, rs3x, rs4, xs, back_s, back_r, low_s, low_r, coef, err,
    gb, gbs, gb1, gb2s, gb2, gb3s, gb3, fin, ls, l1, l2, lz,
    fac, loc, send_s, ag_r, ag_c, rs1_r, rs2_r, rs3_r, rs3x_r, rs4_r,
    x_r, g1_r, g2_r, g3_r, fin_r, l_r, lz_r,
):
    depth = n // 4
    last = depth - 1
    p = lax.axis_index("dp")
    t = lax.axis_index("tensor")
    c, y, z = p % 2, (p // 2) % 2, p // 4
    tokens, ff = act.shape
    rows, rank = a_hbm.shape
    width = grad.shape[1]
    chunk = width // depth

    def at(zz, yy, cc):
        return (zz * 2 + yy) * 2 + cc

    def remote(s, d, ss, rs, dev, tensor=None):
        return pltpu.make_async_remote_copy(
            src_ref=s, dst_ref=d, send_sem=ss, recv_sem=rs,
            device_id=(dev, t if tensor is None else tensor), device_id_type=MESH,
        )

    core, side = at(z, y, 1 - c), at(z, 1 - y, c)

    load_a = pltpu.make_async_copy(a_hbm, a_all.at[pl.ds(pl.multiple_of(p * rows, 16), rows)], loc.at[0])
    load_g = pltpu.make_async_copy(grad_hbm, grad, loc.at[1])
    load_b = pltpu.make_async_copy(b_hbm, b_mat, loc.at[2])
    load_x = pltpu.make_async_copy(act_hbm, act, loc.at[3])
    small = [
        pltpu.make_async_copy(s, d, loc.at[4 + i])
        for i, (s, d) in enumerate(((ratio_hbm, ratio_ref), (len_hbm, len_ref), (rew_hbm, rew_ref)))
    ]
    load_a.start()
    barrier = pltpu.get_barrier_semaphore()
    for dev in [core, side] + [at((z + k) % depth, y, c) for k in range(1, depth)]:
        pl.semaphore_signal(barrier, inc=1, device_id=(dev, t), device_id_type=MESH)
    pl.semaphore_signal(barrier, inc=1, device_id=(p, 1 - t), device_id_type=MESH)
    for copy in [load_g, load_b] + small:
        copy.start()
    load_a.wait()
    load_x.start()
    with jax.named_scope("barrier") if SCOPES else contextlib.nullcontext():
        pl.semaphore_wait(barrier, depth + 2)
    flip = (2 * z > last).astype(jnp.int32)
    tile = tile_of(4 * rows, 1280)
    steps = 4 * rows // tile

    def run(u, own):
        sent = []
        mate = 1 - own

        def m(k):
            return k + flip * (last - 2 * k)

        def dev(k, yy, cc):
            return at(m(k), yy, cc)

        there = 1 - y
        others = sorted((k for k in range(depth) if k != u), key=lambda k: abs(k - u))
        up = u + 1 if u < last else None
        down = u - 1 if u > 0 else None

        def onward(k):
            return up if k < u else down

        def go(s, d, rs, device, tensor=None):
            size = s.dtype.itemsize * math.prod(s.shape) // 256
            if not sent or sent[-1] + size > ff:
                sent.append(0)
            sent[-1] += size
            remote(s, d, send_s.at[len(sent) - 1], rs, device, tensor).start()

        def drain():
            for i, size in enumerate(sent):
                ref = a_all.at[pl.ds(0, size)]
                remote(ref, ref, send_s.at[i], send_s.at[i], core).wait_send()

        def got(d, rs):
            remote(d, d, send_s.at[0], rs, core).wait_recv()

        def z_dev(k):
            return dev(k, y, c)

        middle = cut_g // 32 * 16
        first_rows = [(0, middle), (middle, cut_g)]
        carried = [(own, low, high, True) for low, high in first_rows]
        if own == 1:
            carried += [(cc, cut_g, rows, False) for cc in (1, 0)]

        def rows_of(k, yy, cc, low, high):
            return a_all.at[pl.ds(pl.multiple_of(dev(k, yy, cc) * rows + low, 16), high - low)]

        def piece(k, yy, i):
            return rows_of(k, yy, *carried[i][:3]), ag_r.at[(m(k) * 2 + yy) * 4 + i]

        def a_send(k, yy, i, *devices):
            ref, sem = piece(k, yy, i)
            for device in devices:
                if device is not None:
                    go(ref, ref, sem if device is not core else ag_c.at[m(k) * 2 + yy], device)

        def a_wait(k, yy, i):
            got(*piece(k, yy, i))

        def a_core(k, yy):
            size = cut_g
            if own == 0:
                size = rows if k == u and yy is y else 2 * rows - cut_g
            got(a_all.at[pl.ds(0, size)], ag_c.at[m(k) * 2 + yy])

        up_dev = None if up is None else z_dev(up)
        down_dev = None if down is None else z_dev(down)
        line = (up_dev, down_dev)

        def a_start():
            a_send(u, y, 0, *line)
            if own == 0:
                ref = rows_of(u, y, 0, cut_g, rows)
                go(ref, ref, ag_c.at[2 * depth], core)
                a_send(u, y, 1, *line)
                a_send(u, y, 0, side)
                a_send(u, y, 1, side)
            else:
                a_send(u, y, 2, side)
                a_send(u, y, 1, *line)
                a_send(u, y, 2, *line)
            for i in range(2 + own):
                a_send(u, y, i, core)

        def a_mate():
            got(rows_of(u, y, 0, cut_g, rows), ag_c.at[2 * depth])
            a_send(u, y, 3, side, *line)
            a_send(u, y, 0, side)
            a_send(u, y, 1, side)

        def a_side(i):
            a_wait(u, 1 - y, i)
            if not carried[i][3]:
                a_send(u, 1 - y, i, *line)
            a_send(u, 1 - y, i, core)

        def a_line(k, yy, i):
            a_wait(k, yy, i)
            to = onward(k)
            a_send(k, yy, i, None if to is None else z_dev(to))
            if carried[i][3]:
                a_send(k, yy, i, side)
            a_send(k, yy, i, core)

        def a_over(k, i):
            a_wait(k, 1 - y, i)
            a_send(k, 1 - y, i, core)

        def low_rows(start, size, first=False):
            width_of = size if size <= 2048 else tile_of(size, 1280)

            def step(i, total):
                cols = pl.ds(pl.multiple_of(start + i * width_of, 128), width_of)
                return total + jnp.dot(act[:, cols], a_all[cols, :], preferred_element_type=f32)

            begin = jnp.zeros((tokens, rank), f32) if first else xs[1]
            xs[1] = lax.fori_loop(0, size // width_of, step, begin)

        def low_of(k, first):
            for yy in (y, there):
                a_core(k, yy)
            low_rows(m(k) * (4 * rows), 4 * rows, first)

        small_part = 2 * rows // 128 * 128

        def low_near(k):
            a_core(k, y)
            low_rows(m(k) * (4 * rows) + y * (4 * rows - small_part), small_part)

        def low_far(k):
            a_core(k, 1 - y)
            low_rows(m(k) * (4 * rows) + (1 - y) * small_part, 4 * rows - small_part)

        def low_send():
            low_s[...] = xs[1].astype(bf16)
            go(low_s, low_r, x_r.at[1], p, 1 - t)

        def source_slot(k):
            return z - (z > m(k)).astype(jnp.int32)

        def loss_one():
            go(ls.at[0], l1, l_r.at[0], core)

        def loss_two():
            got(l1, l_r.at[0])
            ls[1] = ls[0] + l1[...]
            go(ls.at[1], l2, l_r.at[1], side)

        def loss_three():
            got(l2, l_r.at[1])
            ls[2] = ls[1] + l2[...]
            for k in others:
                go(ls.at[2], lz.at[source_slot(k)], lz_r.at[0], z_dev(k))

        def loss_end():
            if last:
                got(lz.at[pl.ds(0, last)], lz_r.at[0])
            total = ls[2]
            for i in range(last):
                total = total + lz[i]
            out_loss[...] = fac[...] * total

        def back_send():
            load_g.wait()
            load_b.wait()
            xs[0] = lax.dot_general(
                grad[...], b_mat[...], (((1,), (1,)), ((), ())), preferred_element_type=f32
            )
            back_s[...] = xs[0].astype(bf16)
            go(back_s, back_r, x_r.at[0], p, 1 - t)

        def token_terms_here():
            for copy in small:
                copy.wait()
            per_group = n // groups
            group = p // per_group
            offset = (p % per_group) * tokens
            slots = (
                lax.broadcasted_iota(jnp.int32, ratio_ref.shape, 0) * 128
                + lax.broadcasted_iota(jnp.int32, ratio_ref.shape, 1)
                + offset
            )
            live_total = jnp.int32(0)
            live = jnp.zeros(ratio_ref.shape, f32)
            token_adv = jnp.zeros(ratio_ref.shape, f32)
            for g in range(groups):
                here = jnp.full((1, 128), (group == g).astype(f32))
                reward = [jnp.full((1, 128), rew_ref[g, i]).astype(f32) for i in range(rollouts)]
                center = sum(reward) / rollouts
                spread = sum((r - center) * (r - center) for r in reward) / rollouts
                scale = jnp.sqrt(spread + 1.0)
                end = jnp.int32(0)
                for i in range(rollouts):
                    start = end
                    end = end + len_ref[g, i]
                    member = ((slots >= start) & (slots < end)).astype(f32) * here
                    live = live + member
                    token_adv = token_adv + member * ((reward[i] - center) / scale)
                live_total = live_total + jnp.minimum(end, per_group * tokens)
            ratio = jnp.exp(ratio_ref[...])
            unclipped = ratio * token_adv
            clipped = jnp.clip(ratio, 1.0 - clip_eps, 1.0 + clip_eps) * token_adv
            token_loss = -jnp.minimum(unclipped, clipped)
            slope = jnp.where(unclipped <= clipped, -unclipped, jnp.zeros_like(unclipped))
            weight = live * slope
            for i in range(tokens // 128):
                coef[pl.ds(i * 128, 128), :] = jnp.broadcast_to(weight[i : i + 1, :], (128, 128)).T
            fac[...] = groups / jnp.full((1, 128), live_total).astype(f32)
            loss_part = jnp.sum(jnp.sum(live * token_loss, axis=1, keepdims=True), axis=0, keepdims=True)
            ls[0] = jnp.broadcast_to(loss_part, (8, 128))

        def back_end():
            got(back_r, x_r.at[0])
            err[...] = (adapter_scale_factor * coef[...] * (xs[0] + back_r[...].astype(f32))).astype(bf16)

        def span(k, yy, cc, part_two=None):
            q = dev(k, yy, cc)
            low, size = {None: (0, rows), 0: (0, cut_r), 1: (cut_r, rows - cut_r)}[part_two]
            return part.at[pl.ds(pl.multiple_of(q * rows + low, 16), size)]

        def part_of(k):
            base = m(k) * (4 * rows)

            def step(i, _):
                cols = pl.ds(pl.multiple_of(base + i * tile, 128), tile)
                part[cols, :] = lax.dot_general(
                    act[:, cols], err[...], (((0,), (0,)), ((), ())), preferred_element_type=f32
                ).astype(bf16)
                return 0

            lax.fori_loop(0, steps, step, 0)
            for yy in (1 - y, y):
                slot = m(k) * 2 + yy
                go(span(k, yy, 1 - c), rs1.at[slot], rs1_r.at[m(k)], core)

        def both(k, yy, i):
            low, size = (0, cut_r) if i == 0 else (cut_r, rows - cut_r)
            return span(k, yy, c, i)[...].astype(f32) + rs1[m(k) * 2 + yy, pl.ds(low, size), :].astype(f32)

        def core_wait(k):
            got(rs1.at[pl.ds(m(k) * 2, 2)], rs1_r.at[m(k)])

        def core_sum(k):
            ref = span(k, 1 - y, c, 0)
            ref[...] = both(k, 1 - y, 0).astype(bf16)
            go(ref, rs2.at[m(k)], rs2_r.at[m(k)], side)

        def line_slot(k, upward, final):
            falling = (flip if upward else 1 - flip) if final else 0
            return m(k) + falling * (depth - m(k))

        def sources(k):
            found = []
            if k >= u and down is not None:
                found.append(line_slot(k, True, k == u))
            if k <= u and up is not None:
                found.append(line_slot(k, False, k == u))
            return found

        def line_x(k):
            for slot in sources(k):
                got(rs3x.at[slot], rs3x_r.at[slot])
            for b, yy in enumerate((1 - y, y)):
                total = both(k, yy, 1)
                for slot in sources(k):
                    total = total + rs3x[slot, b].astype(f32)
                ref = span(k, yy, c, 1)
                if k != u:
                    ref[...] = total.astype(bf16)
                    slot = line_slot(k, k > u, abs(k - u) == 1)
                    go(ref, rs3x.at[slot, b], rs3x_r.at[slot], z_dev(up if k > u else down))
                elif b == 0:
                    ref[...] = total.astype(bf16)
                    go(ref, rs4, rs4_r.at[0], side)
                else:
                    out_a[pl.ds(cut_r, rows - cut_r), :] = total

        def line_sum(k):
            got(rs2.at[m(k)], rs2_r.at[m(k)])
            total = both(k, y, 0) + rs2[m(k)].astype(f32)
            for slot in sources(k):
                got(rs3.at[slot], rs3_r.at[slot])
                total = total + rs3[slot].astype(f32)
            if k == u:
                out_a[pl.ds(0, cut_r), :] = fac[...] * total
            else:
                ref = span(k, y, c, 0)
                ref[...] = total.astype(bf16)
                slot = line_slot(k, k > u, abs(k - u) == 1)
                go(ref, rs3.at[slot], rs3_r.at[slot], z_dev(up if k > u else down))

        def a_end():
            got(rs4, rs4_r.at[0])
            rest = pl.ds(cut_r, rows - cut_r)
            out_a[rest, :] = fac[...] * (out_a[rest, :] + rs4[...].astype(f32))

        bases, halves, quarters = (0, rank // 4), (rank // 4, rank * 3 // 4), (rank // 8, rank * 3 // 8)
        lane, other, quarter = bases[own], bases[mate], quarters[own]
        whole = pl.ds(0, quarter)
        away = pl.multiple_of((1 - y) * quarter, 16)
        stay = pl.multiple_of(y * quarter, 16)
        mine = pl.multiple_of(lane + stay, 16)
        b_order = others[::-1] + [u]

        def cols_of(k):
            return pl.ds(pl.multiple_of(m(k) * chunk, 128), chunk)

        def b_part():
            got(low_r, x_r.at[1])
            weighted = coef[...] * (xs[1] + low_r[...].astype(f32))
            high = weighted.astype(bf16)
            rest = (weighted - high.astype(f32)).astype(bf16)
            for k in b_order:
                cols = cols_of(k)
                total = sum(
                    lax.dot_general(w, grad[:, cols], (((0,), (0,)), ((), ())), preferred_element_type=f32)
                    for w in (rest, high)
                )
                gb[:, cols] = total
                gbs[:, cols] = total.astype(bf16)
                rest_rows = pl.ds(0, halves[mate])
                go(gbs.at[pl.ds(other, halves[mate]), cols], gb1.at[rest_rows, cols], g1_r.at[m(k)], core)

        def b_core(k):
            cols = cols_of(k)
            got(gb1.at[pl.ds(0, halves[own]), cols], g1_r.at[m(k)])
            gb2s[whole, cols] = (
                gb[pl.ds(pl.multiple_of(lane + away, 16), quarter), cols]
                + gb1[pl.ds(away, quarter), cols].astype(f32)
            ).astype(bf16)
            go(gb2s.at[whole, cols], gb2.at[whole, cols], g2_r.at[m(k)], side)

        def b_side(k):
            cols = cols_of(k)
            got(gb2.at[whole, cols], g2_r.at[m(k)])
            total = (
                gb[pl.ds(mine, quarter), cols]
                + gb1[pl.ds(stay, quarter), cols].astype(f32)
                + gb2[whole, cols].astype(f32)
            )
            if k == u:
                gb[pl.ds(mine, quarter), cols] = total
            else:
                gb3s[whole, cols] = total.astype(bf16)
                go(gb3s.at[whole, cols], gb3.at[source_slot(k), whole], g3_r.at[0], z_dev(k))

        def final(k, yy, cc):
            at_row = pl.multiple_of(bases[cc] + yy * quarters[cc], 16)
            return fin.at[pl.ds(at_row, quarters[cc]), cols_of(k)], fin_r.at[m(k) * 2 + yy]

        def b_send(k, yy, *devices):
            ref, sem = final(k, yy, own)
            for device in devices:
                go(ref, ref, sem if device is not core else fin_r.at[2 * depth], device)

        def b_line():
            cols = cols_of(u)
            total = gb[pl.ds(mine, quarter), cols]
            if last:
                got(gb3.at[pl.ds(0, last), whole], g3_r.at[0])
            for i in range(last):
                total = total + gb3[i, whole, :].astype(f32)
            scaled = jnp.full((1, 128), adapter_scale_factor) * fac[...]
            fin[pl.ds(mine, quarter), cols] = (scaled[:, :1] * total).astype(bf16)
            b_send(u, y, *[z_dev(k) for k in others[::-1]], side, core)

        def b_pass(k, yy):
            got(*final(k, yy, own))
            if yy is y and abs(k - u) > 1:
                b_send(k, yy, side)
            if k == u:
                b_send(k, yy, *[device for device in (up_dev, down_dev) if device is not None])
            b_send(k, yy, core)

        def b_end():
            got(fin.at[pl.ds(other, halves[mate])], fin_r.at[2 * depth])
            out_b[...] = fin[...].astype(f32)

        plan = [
            (0.0, a_start), (0.1, back_send), (0.2, token_terms_here), (0.3, loss_one), (0.4, load_x.wait),
            (4.55, back_end), (7.2, loss_two), (21.5, loss_three),
        ]
        order = [k for k in (range(last, -1, -1)) if k > u] + [k for k in range(u)] + [u]
        for i, k in enumerate(order):
            plan.append((4.6 + 1.1 * i, part_of, k))
            ready = 7.3 + 1.15 * i
            plan.append((ready, core_wait, k))
            first = ready if i == 0 else (17.35 if u == 0 else 11.35)
            plan.append((max(first, ready) + 0.01 * (i + 1), core_sum, k))
        if u == 0:
            for i, k in enumerate(order[:-1]):
                plan.append((7.35 + 1.15 * i if i < 2 else 15.4, line_x, k))
            plan.append((15.3, line_sum, order[0]))
        else:
            for k in order:
                if k > u:
                    plan.append((15.1 + 4.8 * (last - k), line_x, k))
                    plan.append((21.8 + 8.6 * (last - k), line_sum, k))
                elif k < u:
                    plan.append((21.7, line_x, k))
                    plan.append((30.3, line_sum, k))
                else:
                    plan.append((26.6, line_x, k))
        if own == 0:
            plan += [(4.4, a_side, 0), (6.2, a_side, 1)]
        else:
            plan += [(0.35, a_mate), (2.9, a_side, 2), (4.2, a_side, 3), (6.0, a_side, 0), (7.7, a_side, 1)]
        when = {}
        for core_id in (0, 1):
            moments = {}
            for k in others:
                hops = abs(k - u)
                moments[k] = 4.35 * hops if core_id == 0 else 3.5 + 6.0 * (hops - 1)
            queue, crossing = 4.7, 2.7 if core_id == 0 else 1.8
            arrivals = sorted((moments[k] + 1.7 * i, k, i) for k in others for i in (0, 1))
            for moment, k, i in arrivals:
                queue = max(queue, moment) + 1.75
                when[k, i] = max(when.get((k, i), 0), queue + crossing)
                if core_id == own:
                    plan.append((moment, a_line, k, y, i))
                    plan.append((queue + crossing + 1.0, a_over, k, i))
            if core_id == own == 1:
                for k in others:
                    for i in (2, 3):
                        plan.append((moments[k] + 1.6 + 0.6 * i, a_line, k, y, i))
                        plan.append((moments[k] + 2.8 + 0.6 * i, a_line, k, there, i))
        for i, k in enumerate([u] + others):
            done = 9.0 if i == 0 else when[k, 1] + 1.2 + 0.1 * i
            if i < depth - 1 or depth == 1:
                plan.append((done, low_of, k, i == 0))
            else:
                plan.append((done - 0.6, low_near, k))
                plan.append((done, low_far, k))
        plan.append((done + 0.1, low_send))
        begin = done + 4.5
        if u == 0:
            plan.append((begin + 1.6, line_x, u))
            for k, moment in zip(order[1:-1], (done + 0.15, done + 0.3)):
                plan.append((moment, line_sum, k))
        plan.append((begin, b_part))
        for i, k in enumerate(b_order):
            plan.append((begin + 1.5 + 0.01 * i, b_core, k))
            plan.append((begin + 4.5 + 0.9 * i, b_side, k))
        begin = max(begin, 6.0 * last + 10.3)
        plan.append((begin + 9.5, b_line))
        plan.append((begin + 12.9, line_sum, u))
        plan.append((begin + 12.91, a_end))
        plan.append((begin + 12.0, b_pass, u, there))
        for i, k in enumerate(others):
            plan.append((begin + 12.1 + 0.01 * (last - i), b_pass, k, y))
            plan.append((begin + 14.0 + 0.9 * i, b_pass, k, there))
        plan.append((begin + 18.0, loss_end))
        plan.append((begin + 19.0, b_end))
        for entry in sorted(plan, key=lambda e: e[0]):
            name = getattr(entry[1], "__name__", "w") + "_".join(str(v) for v in entry[2:] if isinstance(v, int))
            with jax.named_scope(name) if SCOPES else contextlib.nullcontext():
                entry[1](*entry[2:])
        with jax.named_scope("drain") if SCOPES else contextlib.nullcontext():
            drain()

    for u in range((depth + 1) // 2):
        for own in (0, 1):
            @pl.when((jnp.minimum(z, last - z) == u) & (c == own))
            def _():
                run(u, own)


def finish_kernel(a_in, b_in, loss_in, a_out, b_out, loss_out, loss_s, sems):
    loss_s[0, 0] = loss_in[0, 0]
    copies = [
        pltpu.make_async_copy(s, d, sems.at[i])
        for i, (s, d) in enumerate(((b_in, b_out), (a_in, a_out), (loss_s, loss_out)))
    ]
    for copy in copies:
        copy.start()
    for copy in copies:
        copy.wait()


def fused_local(activations, output_gradient, adapter_a, adapter_b, log_ratio, lengths, rewards):
    n = lax.axis_size("dp")
    depth = n // 4
    tokens, ff = activations.shape
    rows, rank = adapter_a.shape[1:]
    width = output_gradient.shape[1]
    dma = pltpu.SemaphoreType.DMA
    vmem, anywhere = pl.BlockSpec(memory_space=pltpu.VMEM), pl.BlockSpec(memory_space=pl.ANY)
    scalars = pl.BlockSpec(memory_space=pltpu.SMEM)
    hbm = pl.BlockSpec(memory_space=pltpu.HBM)
    quarter, chunk = rank // 4, width // depth
    quarter = rank * 3 // 8
    cut_g, cut_r = rows * 3 // 64 * 16, rows // 32 * 16
    grad_a, grad_b, loss = pl.pallas_call(
        functools.partial(fused_kernel, n, lengths.shape[0], lengths.shape[1], cut_g, cut_r),
        out_shape=(
            jax.ShapeDtypeStruct((rows, rank), f32),
            jax.ShapeDtypeStruct((rank, width), f32),
            jax.ShapeDtypeStruct((8, 128), f32),
        ),
        in_specs=[hbm] * 7,
        out_specs=(vmem, vmem, vmem),
        scratch_shapes=[
            pltpu.VMEM((tokens // 128, 128), f32),
            pltpu.SMEM(lengths.shape, jnp.int32),
            pltpu.SMEM(rewards.shape, jnp.int32),
            pltpu.VMEM((tokens, ff), bf16),
            pltpu.VMEM((tokens, width), bf16),
            pltpu.VMEM((rank, width), bf16),
            pltpu.VMEM((ff, rank), bf16),
            pltpu.VMEM((ff, rank), bf16),
            pltpu.VMEM((2 * depth, rows, rank), bf16),
            pltpu.VMEM((depth, cut_r, rank), bf16),
            pltpu.VMEM((depth + 1, cut_r, rank), bf16),
            pltpu.VMEM((depth + 1, 2, rows - cut_r, rank), bf16),
            pltpu.VMEM((rows - cut_r, rank), bf16),
            pltpu.VMEM((2, tokens, rank), f32),
            pltpu.VMEM((tokens, rank), bf16),
            pltpu.VMEM((tokens, rank), bf16),
            pltpu.VMEM((tokens, rank), bf16),
            pltpu.VMEM((tokens, rank), bf16),
            pltpu.VMEM((tokens, rank), f32),
            pltpu.VMEM((tokens, rank), bf16),
            pltpu.VMEM((rank, width), f32),
            pltpu.VMEM((rank, width), bf16),
            pltpu.VMEM((rank * 3 // 4, width), bf16),
            pltpu.VMEM((quarter, width), bf16),
            pltpu.VMEM((quarter, width), bf16),
            pltpu.VMEM((quarter, width), bf16),
            pltpu.VMEM((depth, quarter, chunk), bf16),
            pltpu.VMEM((rank, width), bf16),
            pltpu.VMEM((3, 8, 128), f32),
            pltpu.VMEM((8, 128), f32),
            pltpu.VMEM((8, 128), f32),
            pltpu.VMEM((depth, 8, 128), f32),
            pltpu.VMEM((1, 128), f32),
            dma((7,)), dma((4,)), dma((8 * depth,)), dma((2 * depth + 1,)),
            dma((depth,)), dma((depth,)), dma((depth + 1,)), dma((depth + 1,)), dma((1,)),
            dma((2,)), dma((depth,)), dma((depth,)), dma((1,)), dma((2 * depth + 1,)),
            dma((2,)), dma((1,)),
        ],
        compiler_params=pltpu.CompilerParams(
            collective_id=0, has_side_effects=True, vmem_limit_bytes=48 * 1024 * 1024
        ),
        name="fused",
    )(
        *(
            pltpu.with_memory_space_constraint(v, pltpu.HBM)
            for v in (
                activations, output_gradient, adapter_a[0], adapter_b,
                log_ratio.reshape(-1, 128), lengths, rewards,
            )
        )
    )
    grad_a, grad_b, loss = pl.pallas_call(
        finish_kernel,
        out_shape=(
            jax.ShapeDtypeStruct((rows, rank), f32),
            jax.ShapeDtypeStruct((rank, width), f32),
            jax.ShapeDtypeStruct((1, 1), f32),
        ),
        in_specs=[vmem, vmem, vmem],
        out_specs=(hbm, hbm, hbm),
        scratch_shapes=[pltpu.SMEM((1, 1), f32), dma((3,))],
        compiler_params=pltpu.CompilerParams(vmem_limit_bytes=4 * 1024 * 1024),
        name="finish",
    )(grad_a, grad_b, loss)
    return grad_a[None], grad_b, loss.reshape(())


def fits(mesh):
    n, split = mesh.shape["dp"], mesh.shape["tensor"]
    return n % 4 == 0 and 4 <= n <= 16 and split == 2


def local(activations, output_gradient, adapter_a, adapter_b, log_ratio, lengths, rewards):
    n = lax.axis_size("dp")
    rows, rank = adapter_a.shape[1:]
    width, ff = output_gradient.shape[1], activations.shape[1]
    small = 2 * activations.size + 8 * ff * rank < 32 * 1024 * 1024
    aligned = (
        rows % 16 == 0
        and rank == 128
        and activations.shape[0] % 128 == 0
        and ff % 128 == 0
        and 4 * rows % 128 == 0
        and rows % 32 == 0
        and rows >= 64
        and width % (128 * (n // 4)) == 0
        and n % lengths.shape[0] == 0
    )
    run = fused_local if small and aligned else plain_local
    return run(activations, output_gradient, adapter_a, adapter_b, log_ratio, lengths, rewards)


def solution(mesh):
    in_specs = (
        P("dp", "tensor"),
        P("dp", "tensor"),
        P("tensor", "dp", None),
        P(None, "tensor"),
        P("dp"),
        P(),
        P(),
    )
    out_specs = (P("tensor", "dp", None), P(None, "tensor"), P())
    body = local if fits(mesh) else plain_local
    return jax.shard_map(body, mesh=mesh, in_specs=in_specs, out_specs=out_specs, check_vma=False)
```
